32 devices in a mesh: tm: 4 (over y, core), lev: 8 (over z, x).
Axes of the slice: x: 2, y: 2, z: 4, core: 2. Of those that a mesh axis runs over, the one named last changes fastest.
Arguments:
- obs_cell: int32 [4, 16384], P('tm'), may hold values from 0 to 65535
- innovation: float32 [4, 64, 16384], P('tm', 'lev'), may hold values from -8 to 8
- tangent: float32 [4, 64, 128, 512], P('tm', 'lev'), may hold values from -0.45 to 0.45
- damping: float32 [4, 64, 128], P('tm'), may hold values from 0.05 to 0.95
- spread: float32 [64, 128], replicated, may hold values from 0.5 to 2
- vertical: float32 [64, 64], replicated, may hold values from -0.75 to 0.75
Outputs:
- gradient: float32 [64, 128, 2, 128], P(None, 'lev', None, 'tm')
The draws below stay inside these ranges and needn't reach their ends.
All inputs are finite; a program needn't handle non-finite values.
Results may differ from the reference program's by a relative error of at most 0.0003.
Values sent between devices are 32-bit elements; how exact they have to be, the bound alone decides.
A program may use at most 128 MiB of HBM per device.

```python
import math
import jax
import jax.numpy as jnp
from jax import lax

NLAT = 128
NLON = 512
WAVES = 128
LEVELS = 64
OBS = 16384
TIMES = 4


def touch_ends(drawn, stream_key, smallest, top_value):
    index_at = [jax.random.randint(jax.random.fold_in(stream_key, axis), (), 0, length) for axis, length in enumerate(drawn.shape)]
    widest = drawn.shape.index(max(drawn.shape))
    next_to = index_at[:widest] + [(index_at[widest] + 1) % drawn.shape[widest]] + index_at[widest + 1:]
    return drawn.at[tuple(index_at)].set(smallest).at[tuple(next_to)].set(top_value)


def block_scale(own_key, dims, cuts, smallest, largest):
    gain = 1.0
    for position, shards_of in cuts:
        draws = jax.random.uniform(jax.random.fold_in(jax.random.fold_in(own_key, 6), position), (shards_of,), jnp.float32, smallest / len(cuts), largest / len(cuts))
        gain = gain * jnp.repeat(jnp.exp(draws), dims[position] // shards_of).reshape((-1,) + (1,) * (len(dims) - 1 - position))
    return gain


def bell_draw(key, shape, scale, most, shards=(), held_as=jnp.bfloat16):
    loudness = block_scale(key, shape, shards, -0.22, 0.18) if shards else 1.0
    entries = jax.random.normal(key, shape, jnp.float32) * scale * loudness
    return jnp.minimum(jnp.maximum(entries, -most), most).astype(held_as)


def setup_inputs(seed: int = 0) -> dict:
    key_of = jax.random.split(jax.random.key(seed), 7)
    obs_cell = touch_ends(jax.random.randint(key_of[0], (TIMES, OBS), 0, NLAT * NLON), jax.random.fold_in(key_of[0], 1), 0, (NLAT * NLON) - 1).astype(jnp.int32)
    innovation = bell_draw(key_of[1], (TIMES, LEVELS, OBS), 1.5, 8.0, ((0, 4), (1, 8)), jnp.float32)
    tangent = jnp.clip(jax.random.uniform(key_of[2], (TIMES, LEVELS, NLAT, NLON), jnp.float32, -0.45, 0.45) * block_scale(key_of[2], (TIMES, LEVELS, NLAT, NLON), ((0, 4), (1, 8)), -0.4, 0.0), -0.45, 0.45)
    damping = jnp.clip(jnp.exp(math.log(0.95) - 2.944439 * jax.random.uniform(key_of[3], (TIMES, LEVELS, WAVES), jnp.float32) ** block_scale(key_of[3], (TIMES, LEVELS, WAVES), ((0, 4),), -0.2, 0.2)), 0.05, 0.95)
    spread = jnp.clip(jnp.exp(jax.random.uniform(key_of[4], (LEVELS, WAVES), jnp.float32, math.log(0.5), math.log(2.0))), 0.5, 2.0)
    vertical = bell_draw(key_of[5], (LEVELS, LEVELS), LEVELS ** -0.5, 0.75, (), jnp.float32)
    return dict(obs_cell=obs_cell, innovation=innovation, tangent=tangent, damping=damping, spread=spread, vertical=vertical)


PRECISE = lax.Precision.HIGHEST
HALF_GAMMA_LOG = 0.5 * math.log(math.pi) - math.log(2.0)

def fourier_table(lon_count, wave_count):
    longitude = jnp.arange(lon_count, dtype=jnp.int32)[:, None]
    wavenumber = jnp.arange(wave_count, dtype=jnp.int32)[None, :]
    angles = (longitude * wavenumber % lon_count).astype(jnp.float32) * (2.0 * math.pi / lon_count)
    norm_factor = math.sqrt(2.0 / lon_count)
    columns = jnp.stack([jnp.cos(angles), jnp.sin(angles)], axis=2) * norm_factor
    return columns.reshape(lon_count, 2 * wave_count)

def legendre_table(first_wave, wave_block, lat_count, wave_count):
    orders = (first_wave + jnp.arange(wave_block, dtype=jnp.int32)).astype(jnp.float32)[:, None]
    row_index = jnp.arange(lat_count, dtype=jnp.float32)
    latitude = (row_index + 0.5) * (math.pi / lat_count) - 0.5 * math.pi
    sine_lat = jnp.sin(latitude)[None, :]
    cosine = jnp.cos(latitude)[None, :]
    logdiag = -0.5 * math.log(2.0) + 0.5 * (jax.scipy.special.gammaln(orders + 1.5) - HALF_GAMMA_LOG - jax.scipy.special.gammaln(orders + 1.0)) + orders * jnp.log(cosine)
    diagonal = jnp.exp(logdiag)

    def advance(state_pair, degree):
        prev_one, prev_two = state_pair
        upward = jnp.sqrt(jnp.maximum(4.0 * degree * degree - 1.0, 1.0) / jnp.maximum(degree * degree - orders * orders, 1.0))
        lower = degree - 1.0
        downward = jnp.sqrt(jnp.maximum(lower * lower - orders * orders, 0.0) / jnp.maximum(4.0 * lower * lower - 1.0, 1.0))
        recurred = upward * (sine_lat * prev_one - downward * prev_two)
        current = jnp.where(degree < orders, 0.0, jnp.where(degree == orders, diagonal, recurred))
        return ((current, prev_one), current)
    zero_rows = jnp.zeros((wave_block, lat_count), jnp.float32)
    degrees = jnp.arange(wave_count, dtype=jnp.float32)
    _, values = lax.scan(advance, (zero_rows, zero_rows), degrees, unroll=16)
    weight = jnp.sqrt(math.pi / lat_count * cosine)
    return values * weight[None]

def forcing_field(cell_ids, innov_rows, lat_count, lon_count):
    flat_field = jnp.zeros((innov_rows.shape[0], lat_count * lon_count), jnp.float32)
    flat_field = flat_field.at[:, cell_ids].add(innov_rows)
    return flat_field.reshape(innov_rows.shape[0], lat_count, lon_count)

def reference(obs_cell, innovation, tangent, damping, spread, vertical):
    fourier = fourier_table(NLON, WAVES)
    legendre = legendre_table(0, WAVES, NLAT, WAVES)
    adjoint = jnp.zeros((LEVELS, NLAT, NLON), jnp.float32)
    total = jnp.zeros((LEVELS, WAVES, 2, WAVES), jnp.float32)
    for time_step in range(TIMES - 1, -1, -1):
        forced = adjoint + forcing_field(obs_cell[time_step], innovation[time_step], NLAT, NLON)
        coeffs = jnp.einsum('klx,xc->klc', forced, fourier, precision=PRECISE)
        coeffs = coeffs.reshape(LEVELS, NLAT, WAVES, 2)
        spectral = jnp.einsum('klmp,nml->kmpn', coeffs, legendre, precision=PRECISE)
        total = total + spectral
        filtered = spectral * damping[time_step][:, None, None, :]
        synthesized = jnp.einsum('kmpn,nml->klmp', filtered, legendre, precision=PRECISE)
        synthesized = synthesized.reshape(LEVELS, NLAT, 2 * WAVES)
        adjoint = tangent[time_step] * forced + jnp.einsum('klc,xc->klx', synthesized, fourier, precision=PRECISE)
    scaled = total * spread[:, None, None, :]
    return jnp.einsum('kj,kmpn->jmpn', vertical, scaled, precision=PRECISE)
```

```python
import functools
import math

import jax
import jax.numpy as jnp
import numpy as np
from jax import lax
from jax.experimental import pallas as pl
from jax.experimental.pallas import tpu as pltpu
from jax.sharding import PartitionSpec as P

PRECISE = lax.Precision.HIGHEST
BF16 = jnp.bfloat16
F32 = jnp.float32
NT = (((1,), (1,)), ((), ()))
NN = (((1,), (0,)), ((), ()))
VMEM_BYTES = 62 * 1024 * 1024
LANES = 128


def dot(left, right, dims):
    return lax.dot_general(left, right, dims, preferred_element_type=F32)


def halves(value):
    high = value.astype(BF16)
    return high, (value - high.astype(F32)).astype(BF16)


def fourier_rows(lon_count, wave_count):
    index = np.arange(wave_count)[:, None] * np.arange(lon_count)[None, :] % lon_count
    angles = 2.0 * np.pi * index / lon_count
    return (np.concatenate([np.cos(angles), np.sin(angles)], 0) * np.sqrt(2.0 / lon_count)).astype(np.float32)


def legendre_coefficients(lat_count, wave_count):
    half = lat_count // 2
    pack = 2 * LANES // half
    groups = wave_count // pack
    deep = LANES // pack
    phi = (np.arange(half) + 0.5) * np.pi / lat_count - 0.5 * np.pi
    orders = np.arange(wave_count).astype(np.float64)
    lead = np.array(
        [
            -0.5 * math.log(2.0)
            + 0.5 * (math.lgamma(m + 1.5) - math.lgamma(1.5) - math.lgamma(m + 1.0))
            for m in range(wave_count)
        ]
    )
    weight = np.sqrt(np.pi * np.cos(phi) / lat_count)
    diagonal = weight[None, :] * np.exp(lead[:, None] + orders[:, None] * np.log(np.cos(phi))[None, :])
    diagonal = diagonal.reshape(groups, pack * half)
    mu = np.broadcast_to(np.tile(np.sin(phi), pack)[None, :], (groups, pack * half))
    degree = orders[:, None]
    above = degree > orders[None, :]
    gap = np.where(above, degree**2 - orders[None, :] ** 2, 1.0)
    up = np.where(above, np.sqrt(np.maximum(4.0 * degree**2 - 1.0, 0.0) / gap), 0.0)
    lower = degree - 1.0
    down = np.sqrt(np.maximum(lower**2 - orders[None, :] ** 2, 0.0) / np.maximum(4.0 * lower**2 - 1.0, 1.0))

    def packed(a):
        a = a.reshape(wave_count // deep, deep, groups, pack)
        return a.transpose(0, 2, 1, 3).reshape(wave_count // deep * groups, deep * pack)

    return [np.asarray(a, np.float32) for a in (mu, diagonal, packed(up), packed(up * down))]


def forcing_kernel(lat_rows, lon_cols, cell_ref, innov_ref, out_ref):
    cells = cell_ref[0]
    width = cells.shape[1]
    rows = cells // lon_cols
    cols = cells - rows * lon_cols
    innov = innov_ref[0]
    levels = innov.shape[0]
    hit = lax.broadcasted_iota(jnp.int32, (lat_rows, width), 0) == rows
    spread_cols = jnp.where(
        lax.broadcasted_iota(jnp.int32, (lon_cols, width), 0) == cols, 1.0, 0.0
    ).astype(BF16)
    high = innov.astype(BF16).astype(F32)
    low = innov - high
    pieces = [jnp.where(hit, part[k : k + 1, :], 0.0).astype(BF16) for part in (high, low) for k in range(levels)]
    field = dot(jnp.concatenate(pieces, 0), spread_cols, NT)
    field = field[: levels * lat_rows] + field[levels * lat_rows :]

    @pl.when(pl.program_id(1) == 0)
    def _():
        out_ref[0] = field

    @pl.when(pl.program_id(1) > 0)
    def _():
        out_ref[0] += field


def forcing_fields(cells, innov, lat_rows, lon_cols):
    times, levels, count = innov.shape
    width = math.gcd(count, 2048)
    body = functools.partial(forcing_kernel, lat_rows, lon_cols)
    return pl.pallas_call(
        body,
        grid=(times, count // width),
        in_specs=[
            pl.BlockSpec((1, 1, width), lambda t, c: (t, 0, c)),
            pl.BlockSpec((1, levels, width), lambda t, c: (t, 0, c)),
        ],
        out_specs=pl.BlockSpec((1, levels * lat_rows, lon_cols), lambda t, c: (t, 0, 0)),
        out_shape=jax.ShapeDtypeStruct((times, levels * lat_rows, lon_cols), F32),
        compiler_params=pltpu.CompilerParams(vmem_limit_bytes=VMEM_BYTES),
        cost_estimate=pl.CostEstimate(
            flops=4 * times * levels * lat_rows * lon_cols * count, bytes_accessed=8 * 2**20, transcendentals=0
        ),
    )(cells.reshape(times, 1, count), innov)


def lanes_at(value, index):
    return jnp.take_along_axis(value, jnp.broadcast_to(index, value.shape), axis=1, mode="promise_in_bounds")


def sweep_kernel(
    sections, field_ref, tangent_ref, damp_ref, scale_ref, fhigh_ref, flow_ref, mu_ref, diag_ref, up_ref, both_ref,
    out_ref, left, right, high, low, even, odd, packed, total, adjoint, order,
):
    times, rows, lon_cols = field_ref.shape
    groups, width = mu_ref.shape
    waves = high.shape[1]
    lat_rows = width * groups * 2 // waves
    half = lat_rows // 2
    pack = width // half
    deep = LANES // pack
    levels = rows // lat_rows
    group = damp_ref.shape[1]
    mid = group // 2

    lane = lax.broadcasted_iota(jnp.int32, (1, LANES), 1)
    in_first = lane < half
    fold = lane % half
    sub = lax.broadcasted_iota(jnp.int32, (groups, width), 0)
    orders = sub * pack + lax.broadcasted_iota(jnp.int32, (groups, width), 1) // half

    def advance(n, state):
        one, two = state
        place = pl.ds(pl.multiple_of(n // deep * groups, groups), groups)
        base = (n % deep) * pack

        def spread_out(ref):
            value = ref[place, :]
            return jnp.concatenate([lanes_at(value, base + lane // half + i * (LANES // half)) for i in range(width // LANES)], 1)

        recurred = spread_out(up_ref) * (mu_ref[...] * one) - spread_out(both_ref) * two
        value = jnp.where(orders == n, diag_ref[...], recurred)
        row = (n % 2) * (waves // 2) + n // 2
        left[pl.ds(row, groups, stride=waves), :] = value[:, :LANES]
        right[pl.ds(row, groups, stride=waves), :] = value[:, LANES:]
        return value, one

    zero = 0.0 * mu_ref[...]
    lax.fori_loop(0, waves, advance, (zero, zero), unroll=8)

    def split(g, carry):
        for i, ref in enumerate((left, right)):
            upper, lower = halves(ref[pl.ds(pl.multiple_of(g * waves, waves), waves), :])
            high[g, :, i * LANES : (i + 1) * LANES] = upper
            low[g, :, i * LANES : (i + 1) * LANES] = lower
        return carry

    lax.fori_loop(0, groups, split, 0, unroll=4)

    in_high = lax.broadcasted_iota(jnp.int32, (group, LANES), 0) < mid
    n_even = lax.broadcasted_iota(jnp.int32, (group, LANES), 1) < waves // 2
    lat_south = lax.broadcasted_iota(jnp.int32, (group, LANES), 1) < half
    adjoint[...] = jnp.zeros_like(adjoint)
    total[...] = jnp.zeros_like(total)
    own_half = (lax.broadcasted_iota(jnp.int32, (waves, LANES), 1) // half) == (
        lax.broadcasted_iota(jnp.int32, (waves, LANES), 0) % (LANES // half)
    )

    def analyse(t):
        forced = adjoint[...] + field_ref[t]
        adjoint[...] = forced
        upper, lower = halves(forced)
        coeffs = dot(fhigh_ref[...], upper, NT) + dot(flow_ref[...], upper, NT) + dot(fhigh_ref[...], lower, NT)
        for k in range(levels):
            for p in range(2):
                part = coeffs[p * waves : (p + 1) * waves, k * lat_rows : (k + 1) * lat_rows]
                south = lanes_at(part, fold)
                north = lanes_at(part, lat_rows - 1 - fold)
                for value, ref in ((south + north, even), (south - north, odd)):
                    value = jnp.where(own_half, value, 0.0)
                    rounded = value.astype(BF16).astype(F32)
                    ref[pl.ds(2 * k + p, waves, stride=group), :] = rounded
                    ref[pl.ds(mid + 2 * k + p, waves, stride=group), :] = value - rounded

    def pair_sum(value):
        return value + pltpu.roll(value, mid, 0)

    blank = jnp.zeros((group, LANES), F32)
    per_tile = LANES // half

    def place_of(g, i):
        return pl.ds(pl.multiple_of((g * pack + i) * group, group), group)

    def spectral_of(g):
        lefts = []
        for i in range(pack):
            for ref in (even, odd):
                value = ref[place_of(g, i), :]
                tiles = [value if i // per_tile == c else blank for c in range(width // LANES)]
                lefts.append(jnp.concatenate(tiles, 1))
        lefts = jnp.concatenate(lefts, 0).astype(BF16)
        product = dot(lefts, high[g], NT) + dot(lefts, low[g], NT)
        values = []
        for i in range(pack):
            same = product[2 * i * group : (2 * i + 1) * group]
            other = product[(2 * i + 1) * group : (2 * i + 2) * group]
            value = pair_sum(jnp.where(n_even, same, other) if i % 2 == 0 else jnp.where(n_even, other, same))
            total[place_of(g, i), :] += value
            values.append(value)
        return values

    def synthesise(g, values, damp):
        lefts = []
        for i, value in enumerate(values):
            filtered = value * damp
            rounded = filtered.astype(BF16).astype(F32)
            parts = jnp.where(in_high, rounded, filtered - rounded)
            first, second = jnp.where(n_even, parts, 0.0), jnp.where(n_even, 0.0, parts)
            lefts += [first, second] if i % 2 == 0 else [second, first]
        lefts = jnp.concatenate(lefts, 0).astype(BF16)
        product = dot(lefts, high[g], NN) + dot(lefts, low[g], NN)
        for i in range(pack):
            tile = slice(i // per_tile * LANES, (i // per_tile + 1) * LANES)
            same = product[2 * i * group : (2 * i + 1) * group, tile]
            other = product[(2 * i + 1) * group : (2 * i + 2) * group, tile]
            index = (i % per_tile) * half + jnp.where(in_first, lane, lat_rows - 1 - lane)
            same, other = lanes_at(same, index), lanes_at(other, index)
            packed[place_of(g, i), :] = pair_sum(jnp.where(lat_south, same + other, same - other))

    def step(s, carry):
        t = times - 1 - s
        analyse(t)
        damp = damp_ref[t]

        def wave(g, inner):
            synthesise(g, spectral_of(g), damp)
            return inner

        lax.fori_loop(0, groups, wave, 0, unroll=4)
        synth = jnp.concatenate(
            [
                jnp.concatenate([packed[pl.ds(2 * k + p, waves, stride=group), :] for p in range(2)], 0).T
                for k in range(levels)
            ],
            0,
        )
        upper, lower = halves(synth)
        gridded = dot(upper, fhigh_ref[...], NN) + dot(lower, fhigh_ref[...], NN) + dot(upper, flow_ref[...], NN)
        adjoint[...] = tangent_ref[t] * adjoint[...] + gridded
        return carry

    lax.fori_loop(0, times - 1, step, 0)
    analyse(0)

    def last(g, inner):
        spectral_of(g)
        return inner

    lax.fori_loop(0, groups, last, 0, unroll=4)

    block_n = waves // sections
    side = LANES // block_n
    deal = 2 * waves // side
    natural = (lane % 2) * (waves // 2) + lane // 2
    for k in range(levels):
        for p in range(2):
            value = total[pl.ds(2 * k + p, waves, stride=group), :]
            order[pl.ds(p, waves, stride=2), :] = lanes_at(value, natural) * scale_ref[k : k + 1, :]
        blocks = [order[pl.ds(q, deal, stride=side), :] for q in range(side)]
        for s in range(sections):
            value = blocks[0] if s == 0 else pltpu.roll(blocks[0], (-s * block_n) % LANES, 1)
            for q in range(1, side):
                moved = blocks[q] if q == s else pltpu.roll(blocks[q], ((q - s) * block_n) % LANES, 1)
                value = jnp.where(lane // block_n == q, moved, value)
            out_ref[s * levels + k] = value


def sweep(fields, tangent, damp, scale, lat_rows, waves, sections):
    times, rows, lon_cols = fields.shape
    group = damp.shape[1]
    levels = rows // lat_rows
    fourier = fourier_rows(lon_cols, waves)
    fhigh = fourier.astype(jnp.bfloat16)
    flow = (fourier - fhigh.astype(np.float32)).astype(jnp.bfloat16)
    mu, diagonal, up, both = legendre_coefficients(lat_rows, waves)
    groups, width = mu.shape
    return pl.pallas_call(
        functools.partial(sweep_kernel, sections),
        in_specs=[pl.BlockSpec(memory_space=pltpu.VMEM)] * 10,
        out_specs=pl.BlockSpec(memory_space=pltpu.VMEM),
        out_shape=jax.ShapeDtypeStruct((sections * levels, 2 * waves * (waves // sections) // LANES, LANES), F32),
        scratch_shapes=[
            pltpu.VMEM((waves * groups, LANES), F32),
            pltpu.VMEM((waves * groups, LANES), F32),
            pltpu.VMEM((groups, waves, width), BF16),
            pltpu.VMEM((groups, waves, width), BF16),
            pltpu.VMEM((waves * group, LANES), F32),
            pltpu.VMEM((waves * group, LANES), F32),
            pltpu.VMEM((waves * group, LANES), F32),
            pltpu.VMEM((waves * group, LANES), F32),
            pltpu.VMEM((rows, lon_cols), F32),
            pltpu.VMEM((2 * waves, LANES), F32),
        ],
        compiler_params=pltpu.CompilerParams(vmem_limit_bytes=VMEM_BYTES),
    )(fields, tangent, damp, scale, fhigh, flow, mu, diagonal, up, both)


def shards(obs_cell, innovation, tangent, damping, spread, vertical):
    sections = lax.axis_size("tm")
    groups = lax.axis_size("lev")
    me_tm = lax.axis_index("tm")
    me_lev = lax.axis_index("lev")
    lev_dev, lat_rows, lon_cols = tangent.shape[1:]
    levels, waves = damping.shape[1:]
    mine = -(-lev_dev // sections)
    mine += mine % 2
    padded = mine * sections

    def pad_levels(value, axis):
        widths = [(0, 0)] * value.ndim
        widths[axis] = (0, padded - value.shape[axis])
        return jnp.pad(value, widths) if padded > value.shape[axis] else value

    count = obs_cell.shape[1]
    deep = count // LANES
    damp_block = pad_levels(lax.dynamic_slice_in_dim(damping[0], me_lev * lev_dev, lev_dev, 0), 0)
    message = jnp.concatenate(
        [
            pad_levels(innovation[0], 0).reshape(sections, mine * deep, LANES),
            jnp.broadcast_to(obs_cell.astype(F32).reshape(1, deep, LANES), (sections, deep, LANES)),
            damp_block.reshape(sections, mine * waves // LANES, LANES),
        ],
        1,
    )
    message = lax.all_to_all(message, "tm", split_axis=0, concat_axis=0, tiled=True)
    innov = message[:, : mine * deep].reshape(sections, mine, count)
    cells = message[:, mine * deep : (mine + 1) * deep].reshape(sections, count).astype(jnp.int32)
    damp_mine = message[:, (mine + 1) * deep :].reshape(sections, mine, waves)
    rates = lax.all_to_all(
        pad_levels(tangent[0], 0).reshape(sections, mine * lat_rows, lon_cols),
        "tm", split_axis=0, concat_axis=0, tiled=True,
    )
    fields = forcing_fields(cells, innov, lat_rows, lon_cols)
    damp_mine = jnp.concatenate([damp_mine[..., 0::2], damp_mine[..., 1::2]], -1)
    damp_rows = jnp.tile(jnp.repeat(damp_mine, 2, axis=1), (1, 2, 1))
    scale = pad_levels(lax.dynamic_slice_in_dim(spread, me_lev * lev_dev, lev_dev, 0), 0)
    scale = lax.dynamic_slice_in_dim(scale, me_tm * mine, mine, 0)
    total = sweep(fields, rates, damp_rows, scale, lat_rows, waves, sections)

    block_m = waves // groups
    block_n = waves // sections
    deal = total.shape[1] // groups
    outgoing = total.reshape(sections, mine, groups, deal, LANES)
    outgoing = outgoing.transpose(2, 0, 1, 3, 4).reshape(groups * sections, mine * deal, LANES)
    arrived = lax.all_to_all(outgoing, ("lev", "tm"), split_axis=0, concat_axis=0, tiled=True)
    arrived = arrived.reshape(groups, padded, deal * LANES)[:, :lev_dev].reshape(levels, deal * LANES)
    result = jnp.einsum("kj,kx->jx", vertical, arrived, precision=PRECISE)
    return result.reshape(levels, block_m, 2, block_n)


def solution(mesh):
    placed = (
        P("tm", None),
        P("tm", "lev", None),
        P("tm", "lev", None, None),
        P("tm", None, None),
        P(),
        P(),
    )
    return jax.shard_map(
        shards, mesh=mesh, in_specs=placed, out_specs=P(None, "lev", None, "tm"), check_vma=False
    )
```

```python
import functools
import math

import jax
import jax.numpy as jnp
import numpy as np
from jax import lax
from jax.experimental import pallas as pl
from jax.experimental.pallas import tpu as pltpu
from jax.sharding import PartitionSpec as P

PRECISE = lax.Precision.HIGHEST
BF16 = jnp.bfloat16
F32 = jnp.float32
NT = (((1,), (1,)), ((), ()))
NN = (((1,), (0,)), ((), ()))
VMEM_BYTES = 62 * 1024 * 1024
LANES = 128
SUBLANES = 8


def dot(left, right, dims):
    return lax.dot_general(left, right, dims, preferred_element_type=F32)


def halves(value):
    high = value.astype(BF16)
    return high, (value - high.astype(F32)).astype(BF16)


def fourier_rows(lon_count, wave_count):
    index = np.arange(wave_count)[:, None] * np.arange(lon_count)[None, :] % lon_count
    angles = 2.0 * np.pi * index / lon_count
    return (np.concatenate([np.cos(angles), np.sin(angles)], 0) * np.sqrt(2.0 / lon_count)).astype(np.float32)


def legendre_coefficients(lat_count, wave_count):
    half = lat_count // 2
    pack = 2 * LANES // half
    groups = wave_count // pack
    deep = LANES // pack
    phi = (np.arange(half) + 0.5) * np.pi / lat_count - 0.5 * np.pi
    orders = np.arange(wave_count).astype(np.float64)
    lead = np.array(
        [
            -0.5 * math.log(2.0)
            + 0.5 * (math.lgamma(m + 1.5) - math.lgamma(1.5) - math.lgamma(m + 1.0))
            for m in range(wave_count)
        ]
    )
    weight = np.sqrt(np.pi * np.cos(phi) / lat_count)
    diagonal = weight[None, :] * np.exp(lead[:, None] + orders[:, None] * np.log(np.cos(phi))[None, :])
    diagonal = diagonal.reshape(groups, pack * half)
    mu = np.broadcast_to(np.tile(np.sin(phi), pack)[None, :], (groups, pack * half))
    degree = orders[:, None]
    above = degree > orders[None, :]
    gap = np.where(above, degree**2 - orders[None, :] ** 2, 1.0)
    up = np.where(above, np.sqrt(np.maximum(4.0 * degree**2 - 1.0, 0.0) / gap), 0.0)
    lower = degree - 1.0
    down = np.sqrt(np.maximum(lower**2 - orders[None, :] ** 2, 0.0) / np.maximum(4.0 * lower**2 - 1.0, 1.0))

    def packed(a):
        a = a.reshape(wave_count // deep, deep, groups, pack)
        return a.transpose(0, 2, 1, 3).reshape(wave_count // deep * groups, deep * pack)

    return [np.asarray(a, np.float32) for a in (mu, diagonal, packed(up), packed(up * down))]


def bin_shape(lat_rows, lon_cols):
    tall = math.gcd(lat_rows, 32)
    return tall, (lat_rows // tall) * (lon_cols // LANES)


def sort_kernel(
    lon_cols, tall, bins, mine, cell_ref, innov_ref, damp_ref, out_ref, lane_from, sub_from, swaps,
):
    levels, deep, _ = innov_ref.shape
    sections = out_ref.shape[0]
    blocks = deep // SUBLANES
    low_bits, mid_bits, top_bits = (n.bit_length() - 1 for n in (blocks, SUBLANES, LANES))
    mid_end = low_bits + mid_bits
    all_bits = mid_end + top_bits
    lane = lax.broadcasted_iota(jnp.int32, (SUBLANES, LANES), 1)
    sub = lax.broadcasted_iota(jnp.int32, (SUBLANES, LANES), 0)
    span = tall * LANES
    wide = lon_cols // LANES

    def key_of(cells):
        rows = cells // lon_cols
        cols = cells - rows * lon_cols
        tile = (rows // tall) * wide + cols // LANES
        return tile * span + (rows % tall) * LANES + cols % LANES

    keys = [key_of(cell_ref[v * SUBLANES : (v + 1) * SUBLANES, :]) for v in range(blocks)]

    def falling(stage):
        if stage >= all_bits:
            return None
        if stage >= mid_end:
            return (lane >> (stage - mid_end)) & 1
        return (sub >> (stage - low_bits)) & 1

    plan = []

    def across(values, bits, position, axis, stage, first, last):
        down = falling(stage)
        values = [value * (1 << bits) + position for value in values]
        for bit in range(first, last - 1, -1):
            reach = 1 << bit
            index = position ^ reach
            upper = (position >> bit) & 1
            keep = (upper if down is None else upper ^ down) == 0
            moved = []
            for value in values:
                other = jnp.take_along_axis(value, index, axis=axis, mode="promise_in_bounds")
                moved.append(jnp.where(keep, jnp.minimum(value, other), jnp.maximum(value, other)))
            values = moved
        return [value >> bits for value in values], [value & ((1 << bits) - 1) for value in values]

    for stage in range(1, all_bits + 1):
        if stage > mid_end:
            keys, source = across(keys, top_bits, lane, 1, stage, stage - 1 - mid_end, 0)
            slot = sum(1 for kind, _ in plan if kind == "lane")
            for v in range(blocks):
                lane_from[slot, v] = source[v]
            plan.append(("lane", slot))
        if stage > low_bits:
            keys, source = across(keys, mid_bits, sub, 0, stage, min(stage, mid_end) - 1 - low_bits, 0)
            slot = sum(1 for kind, _ in plan if kind == "sub")
            for v in range(blocks):
                sub_from[slot, v] = source[v]
            plan.append(("sub", slot))
        for bit in range(min(stage, low_bits) - 1, -1, -1):
            down = None if stage < low_bits else falling(stage)
            slot = sum(1 for kind, _ in plan if kind == "swap")
            pair = 0
            for v in range(blocks):
                if v >> bit & 1:
                    continue
                first, second = keys[v], keys[v | 1 << bit]
                if stage < low_bits:
                    swap = first < second if v >> stage & 1 else first > second
                elif down is None:
                    swap = first > second
                else:
                    swap = jnp.where(down == 0, first - second, second - first) > 0
                swaps[slot, pair] = jnp.where(swap, 1, 0)
                keys[v], keys[v | 1 << bit] = jnp.where(swap, second, first), jnp.where(swap, first, second)
                pair += 1
            plan.append(("swap", (slot, bit)))

    for s in range(sections):
        out_ref[s, mine * deep : (mine + 1) * deep, :] = jnp.concatenate([key.astype(F32) for key in keys], 0).T

    edges = jnp.zeros((1, LANES), F32)
    for b in range(1, bins + 1):
        below = sum(jnp.where(key < b * span, 1.0, 0.0) for key in keys)
        below = jnp.sum(jnp.sum(below, 0, keepdims=True), 1, keepdims=True)
        edges = jnp.where(lane[:1] == b, below, edges)
    extra = damp_ref.shape[1]
    base = (mine + 1) * deep
    for s in range(sections):
        tail = [damp_ref[s], edges, jnp.zeros((SUBLANES - extra - 1, LANES), F32)]
        out_ref[s, base : base + SUBLANES, :] = jnp.concatenate(tail, 0)
        for k in range(mine):
            if s * mine + k >= levels:
                out_ref[s, k * deep : (k + 1) * deep, :] = jnp.zeros((deep, LANES), F32)

    def move(p, carry):
        values = [innov_ref[p, v * SUBLANES : (v + 1) * SUBLANES, :] for v in range(blocks)]
        for kind, slot in plan:
            if kind == "swap":
                slot, bit = slot
                firsts = [v for v in range(blocks) if not v >> bit & 1]
                for pair, v in enumerate(firsts):
                    swap = swaps[slot, pair] != 0
                    first, second = values[v], values[v | 1 << bit]
                    values[v] = jnp.where(swap, second, first)
                    values[v | 1 << bit] = jnp.where(swap, first, second)
            else:
                ref, axis = (lane_from, 1) if kind == "lane" else (sub_from, 0)
                values = [
                    jnp.take_along_axis(value, ref[slot, v], axis=axis, mode="promise_in_bounds")
                    for v, value in enumerate(values)
                ]
        out_ref[p // mine, pl.ds(pl.multiple_of(p % mine * deep, deep), deep), :] = jnp.concatenate(values, 0).T
        return carry

    lax.fori_loop(0, levels, move, 0)


def sorted_message(cells, innov, damp, mine, lat_rows, lon_cols):
    levels, deep, _ = innov.shape
    sections, extra, _ = damp.shape
    blocks = deep // SUBLANES
    low_bits, mid_bits, top_bits = (n.bit_length() - 1 for n in (blocks, SUBLANES, LANES))
    all_bits = low_bits + mid_bits + top_bits
    tall, bins = bin_shape(lat_rows, lon_cols)
    swap_count = sum(min(stage, low_bits) for stage in range(1, all_bits + 1))
    return pl.pallas_call(
        functools.partial(sort_kernel, lon_cols, tall, bins, mine),
        in_specs=[pl.BlockSpec(memory_space=pltpu.VMEM)] * 3,
        out_specs=pl.BlockSpec(memory_space=pltpu.VMEM),
        out_shape=jax.ShapeDtypeStruct((sections, (mine + 1) * deep + SUBLANES, LANES), F32),
        scratch_shapes=[
            pltpu.VMEM((top_bits, blocks, SUBLANES, LANES), jnp.int32),
            pltpu.VMEM((top_bits + mid_bits, blocks, SUBLANES, LANES), jnp.int32),
            pltpu.VMEM((swap_count, max(1, blocks // 2), SUBLANES, LANES), jnp.int32),
        ],
        compiler_params=pltpu.CompilerParams(vmem_limit_bytes=VMEM_BYTES // 2),
        cost_estimate=pl.CostEstimate(flops=2**30, bytes_accessed=2**21, transcendentals=0),
    )(cells, innov, damp)


def forcing_kernel(mine, tall, edge_ref, message_ref, out_ref):
    times = message_ref.shape[0]
    bins = out_ref.shape[1]
    deep = (message_ref.shape[1] - SUBLANES) // (mine + 1)
    chunks = deep // 2
    span = tall * LANES
    stride = edge_ref.shape[0] // times
    out_ref[...] = jnp.zeros_like(out_ref)
    col_ids = lax.broadcasted_iota(jnp.int32, (LANES, 2 * LANES), 0).astype(F32).astype(BF16)
    row_ids = lax.broadcasted_iota(jnp.int32, (tall, 2 * LANES), 0).astype(F32).astype(BF16)
    one, none = jnp.ones((), BF16), jnp.zeros((), BF16)

    def row_of(t, base, c):
        return jnp.concatenate([message_ref[t, pl.ds(base + 2 * c + i, 1), :] for i in range(2)], 1)

    def visit(t, b, c, live):
        key = row_of(t, mine * deep, c).astype(jnp.int32) - jnp.where(live, b, bins + 1) * span
        cols = (key & (LANES - 1)).astype(F32).astype(BF16)
        rows = (key >> 7).astype(F32).astype(BF16)
        spread_cols = jnp.where(col_ids == jnp.broadcast_to(cols, col_ids.shape), one, none)
        hit = row_ids == jnp.broadcast_to(rows, row_ids.shape)
        parts = [halves(row_of(t, k * deep, c)) for k in range(mine)]
        pieces = [jnp.where(hit, jnp.broadcast_to(part[i], row_ids.shape), none) for i in range(2) for part in parts]
        field = dot(jnp.concatenate(pieces, 0), spread_cols, NT)
        return field[: mine * tall] + field[mine * tall :]

    total = chunks + bins - 1
    unroll = 4

    def walk(s, state):
        fields, nexts = [], []
        for t in range(times):
            b, c = state[t]
            for u in range(unroll):
                live = s * unroll + u < total
                fields.append((t, b, visit(t, b, c, live)))
                stay = edge_ref[t * stride + b + 1] > (c + 1) * 2 * LANES
                b, c = (
                    jnp.minimum(jnp.where(stay, b, b + 1), bins - 1),
                    jnp.minimum(jnp.where(stay, c + 1, c), chunks - 1),
                )
            nexts.append((b, c))
        for t, b, field in fields:
            out_ref[t, b] += field
        return tuple(nexts)

    start = jnp.int32(0)
    lax.fori_loop(0, -(-total // unroll), walk, tuple((start, start) for _ in range(times)))


def forcing_fields(message, edges, mine, lat_rows, lon_cols):
    times = message.shape[0]
    tall, bins = bin_shape(lat_rows, lon_cols)
    return pl.pallas_call(
        functools.partial(forcing_kernel, mine, tall),
        in_specs=[pl.BlockSpec(memory_space=pltpu.SMEM), pl.BlockSpec(memory_space=pltpu.VMEM)],
        out_specs=pl.BlockSpec(memory_space=pltpu.VMEM),
        out_shape=jax.ShapeDtypeStruct((times, bins, mine * tall, LANES), F32),
        compiler_params=pltpu.CompilerParams(vmem_limit_bytes=VMEM_BYTES // 2),
        cost_estimate=pl.CostEstimate(flops=2**33, bytes_accessed=2**22, transcendentals=0),
    )(edges, message)


def lanes_at(value, index):
    return jnp.take_along_axis(value, jnp.broadcast_to(index, value.shape), axis=1, mode="promise_in_bounds")


def sweep_kernel(
    sections, field_ref, tangent_ref, damp_ref, scale_ref, fhigh_ref, flow_ref, mu_ref, diag_ref, up_ref, both_ref,
    out_ref, left, right, high, low, even, odd, packed, total, adjoint, order,
):
    times, rows, lon_cols = tangent_ref.shape
    bins = field_ref.shape[1]
    groups, width = mu_ref.shape
    waves = high.shape[1]
    lat_rows = width * groups * 2 // waves
    half = lat_rows // 2
    pack = width // half
    deep = LANES // pack
    levels = rows // lat_rows
    tall = field_ref.shape[2] // levels
    across = lon_cols // LANES
    group = damp_ref.shape[1]
    mid = group // 2

    lane = lax.broadcasted_iota(jnp.int32, (1, LANES), 1)
    in_first = lane < half
    fold = lane % half
    sub = lax.broadcasted_iota(jnp.int32, (groups, width), 0)
    orders = sub * pack + lax.broadcasted_iota(jnp.int32, (groups, width), 1) // half

    def advance(n, state):
        one, two = state
        place = pl.ds(pl.multiple_of(n // deep * groups, groups), groups)
        base = (n % deep) * pack

        def spread_out(ref):
            value = ref[place, :]
            return jnp.concatenate([lanes_at(value, base + lane // half + i * (LANES // half)) for i in range(width // LANES)], 1)

        recurred = spread_out(up_ref) * (mu_ref[...] * one) - spread_out(both_ref) * two
        value = jnp.where(orders == n, diag_ref[...], recurred)
        row = (n % 2) * (waves // 2) + n // 2
        left[pl.ds(row, groups, stride=waves), :] = value[:, :LANES]
        right[pl.ds(row, groups, stride=waves), :] = value[:, LANES:]
        return value, one

    zero = 0.0 * mu_ref[...]
    lax.fori_loop(0, waves, advance, (zero, zero), unroll=8)

    def split(g, carry):
        for i, ref in enumerate((left, right)):
            upper, lower = halves(ref[pl.ds(pl.multiple_of(g * waves, waves), waves), :])
            high[g, :, i * LANES : (i + 1) * LANES] = upper
            low[g, :, i * LANES : (i + 1) * LANES] = lower
        return carry

    lax.fori_loop(0, groups, split, 0, unroll=4)

    in_high = lax.broadcasted_iota(jnp.int32, (group, LANES), 0) < mid
    n_even = lax.broadcasted_iota(jnp.int32, (group, LANES), 1) < waves // 2
    lat_south = lax.broadcasted_iota(jnp.int32, (group, LANES), 1) < half
    adjoint[...] = jnp.zeros_like(adjoint)
    total[...] = jnp.zeros_like(total)
    own_half = (lax.broadcasted_iota(jnp.int32, (waves, LANES), 1) // half) == (
        lax.broadcasted_iota(jnp.int32, (waves, LANES), 0) % (LANES // half)
    )

    def analyse(t):
        field = [
            jnp.concatenate([field_ref[t, h + i, k * tall : (k + 1) * tall, :] for i in range(across)], 1)
            for k in range(levels)
            for h in range(0, bins, across)
        ]
        forced = adjoint[...] + jnp.concatenate(field, 0)
        adjoint[...] = forced
        upper, lower = halves(forced)
        coeffs = dot(fhigh_ref[...], upper, NT) + dot(flow_ref[...], upper, NT) + dot(fhigh_ref[...], lower, NT)
        for k in range(levels):
            for p in range(2):
                part = coeffs[p * waves : (p + 1) * waves, k * lat_rows : (k + 1) * lat_rows]
                south = lanes_at(part, fold)
                north = lanes_at(part, lat_rows - 1 - fold)
                for value, ref in ((south + north, even), (south - north, odd)):
                    value = jnp.where(own_half, value, 0.0)
                    rounded = value.astype(BF16).astype(F32)
                    ref[pl.ds(2 * k + p, waves, stride=group), :] = rounded
                    ref[pl.ds(mid + 2 * k + p, waves, stride=group), :] = value - rounded

    def pair_sum(value):
        return value + pltpu.roll(value, mid, 0)

    blank = jnp.zeros((group, LANES), F32)
    per_tile = LANES // half

    def place_of(g, i):
        return pl.ds(pl.multiple_of((g * pack + i) * group, group), group)

    def spectral_of(g):
        lefts = []
        for i in range(pack):
            for ref in (even, odd):
                value = ref[place_of(g, i), :]
                tiles = [value if i // per_tile == c else blank for c in range(width // LANES)]
                lefts.append(jnp.concatenate(tiles, 1))
        lefts = jnp.concatenate(lefts, 0).astype(BF16)
        product = dot(lefts, high[g], NT) + dot(lefts, low[g], NT)
        values = []
        for i in range(pack):
            same = product[2 * i * group : (2 * i + 1) * group]
            other = product[(2 * i + 1) * group : (2 * i + 2) * group]
            value = pair_sum(jnp.where(n_even, same, other) if i % 2 == 0 else jnp.where(n_even, other, same))
            total[place_of(g, i), :] += value
            values.append(value)
        return values

    def synthesise(g, values, damp):
        lefts = []
        for i, value in enumerate(values):
            filtered = value * damp
            rounded = filtered.astype(BF16).astype(F32)
            parts = jnp.where(in_high, rounded, filtered - rounded)
            first, second = jnp.where(n_even, parts, 0.0), jnp.where(n_even, 0.0, parts)
            lefts += [first, second] if i % 2 == 0 else [second, first]
        lefts = jnp.concatenate(lefts, 0).astype(BF16)
        product = dot(lefts, high[g], NN) + dot(lefts, low[g], NN)
        for i in range(pack):
            tile = slice(i // per_tile * LANES, (i // per_tile + 1) * LANES)
            same = product[2 * i * group : (2 * i + 1) * group, tile]
            other = product[(2 * i + 1) * group : (2 * i + 2) * group, tile]
            index = (i % per_tile) * half + jnp.where(in_first, lane, lat_rows - 1 - lane)
            same, other = lanes_at(same, index), lanes_at(other, index)
            packed[place_of(g, i), :] = pair_sum(jnp.where(lat_south, same + other, same - other))

    def step(s, carry):
        t = times - 1 - s
        analyse(t)
        damp = damp_ref[t]

        def wave(g, inner):
            for i, value in enumerate(spectral_of(g)):
                packed[place_of(g, i), :] = value
            return inner

        def back(g, inner):
            synthesise(g, [packed[place_of(g, i), :] for i in range(pack)], damp)
            return inner

        lax.fori_loop(0, groups, wave, 0, unroll=32)
        lax.fori_loop(0, groups, back, 0, unroll=32)
        synth = jnp.concatenate(
            [
                jnp.concatenate([packed[pl.ds(2 * k + p, waves, stride=group), :] for p in range(2)], 0).T
                for k in range(levels)
            ],
            0,
        )
        upper, lower = halves(synth)
        gridded = dot(upper, fhigh_ref[...], NN) + dot(lower, fhigh_ref[...], NN) + dot(upper, flow_ref[...], NN)
        adjoint[...] = tangent_ref[t] * adjoint[...] + gridded
        return carry

    lax.fori_loop(0, times - 1, step, 0)
    analyse(0)

    def last(g, inner):
        spectral_of(g)
        return inner

    lax.fori_loop(0, groups, last, 0, unroll=32)

    block_n = waves // sections
    side = LANES // block_n
    deal = 2 * waves // side
    natural = (lane % 2) * (waves // 2) + lane // 2
    for k in range(levels):
        for p in range(2):
            value = total[pl.ds(2 * k + p, waves, stride=group), :]
            order[pl.ds(p, waves, stride=2), :] = lanes_at(value, natural) * scale_ref[k : k + 1, :]
        blocks = [order[pl.ds(q, deal, stride=side), :] for q in range(side)]
        for s in range(sections):
            value = blocks[0] if s == 0 else pltpu.roll(blocks[0], (-s * block_n) % LANES, 1)
            for q in range(1, side):
                moved = blocks[q] if q == s else pltpu.roll(blocks[q], ((q - s) * block_n) % LANES, 1)
                value = jnp.where(lane // block_n == q, moved, value)
            out_ref[s * levels + k] = value


def sweep(fields, tangent, damp, scale, lat_rows, waves, sections):
    times, rows, lon_cols = tangent.shape
    group = damp.shape[1]
    levels = rows // lat_rows
    fourier = fourier_rows(lon_cols, waves)
    fhigh = fourier.astype(jnp.bfloat16)
    flow = (fourier - fhigh.astype(np.float32)).astype(jnp.bfloat16)
    mu, diagonal, up, both = legendre_coefficients(lat_rows, waves)
    groups, width = mu.shape
    return pl.pallas_call(
        functools.partial(sweep_kernel, sections),
        in_specs=[pl.BlockSpec(memory_space=pltpu.VMEM)] * 10,
        out_specs=pl.BlockSpec(memory_space=pltpu.VMEM),
        out_shape=jax.ShapeDtypeStruct((sections * levels, 2 * waves * (waves // sections) // LANES, LANES), F32),
        scratch_shapes=[
            pltpu.VMEM((waves * groups, LANES), F32),
            pltpu.VMEM((waves * groups, LANES), F32),
            pltpu.VMEM((groups, waves, width), BF16),
            pltpu.VMEM((groups, waves, width), BF16),
            pltpu.VMEM((waves * group, LANES), F32),
            pltpu.VMEM((waves * group, LANES), F32),
            pltpu.VMEM((waves * group, LANES), F32),
            pltpu.VMEM((waves * group, LANES), F32),
            pltpu.VMEM((rows, lon_cols), F32),
            pltpu.VMEM((2 * waves, LANES), F32),
        ],
        compiler_params=pltpu.CompilerParams(vmem_limit_bytes=VMEM_BYTES),
    )(fields, tangent, damp, scale, fhigh, flow, mu, diagonal, up, both)


def shards(obs_cell, innovation, tangent, damping, spread, vertical):
    sections = lax.axis_size("tm")
    groups = lax.axis_size("lev")
    me_tm = lax.axis_index("tm")
    me_lev = lax.axis_index("lev")
    lev_dev, lat_rows, lon_cols = tangent.shape[1:]
    levels, waves = damping.shape[1:]
    mine = -(-lev_dev // sections)
    mine += mine % 2
    padded = mine * sections

    def pad_levels(value, axis):
        widths = [(0, 0)] * value.ndim
        widths[axis] = (0, padded - value.shape[axis])
        return jnp.pad(value, widths) if padded > value.shape[axis] else value

    count = obs_cell.shape[1]
    deep = count // LANES
    damp_block = pad_levels(lax.dynamic_slice_in_dim(damping[0], me_lev * lev_dev, lev_dev, 0), 0)
    message = sorted_message(
        obs_cell.reshape(deep, LANES),
        innovation.reshape(lev_dev, deep, LANES),
        damp_block.reshape(sections, mine * waves // LANES, LANES),
        mine,
        lat_rows,
        lon_cols,
    )
    message = lax.all_to_all(message, "tm", split_axis=0, concat_axis=0, tiled=True)
    base = (mine + 1) * deep
    extra = mine * waves // LANES
    damp_mine = message[:, base : base + extra].reshape(sections, mine, waves)
    edges = message[:, base + extra].astype(jnp.int32).reshape(sections * LANES)
    rates = lax.all_to_all(
        pad_levels(tangent[0], 0).reshape(sections, mine * lat_rows, lon_cols),
        "tm", split_axis=0, concat_axis=0, tiled=True,
    )
    fields = forcing_fields(message, edges, mine, lat_rows, lon_cols)
    damp_mine = jnp.concatenate([damp_mine[..., 0::2], damp_mine[..., 1::2]], -1)
    damp_rows = jnp.tile(jnp.repeat(damp_mine, 2, axis=1), (1, 2, 1))
    scale = pad_levels(lax.dynamic_slice_in_dim(spread, me_lev * lev_dev, lev_dev, 0), 0)
    scale = lax.dynamic_slice_in_dim(scale, me_tm * mine, mine, 0)
    total = sweep(fields, rates, damp_rows, scale, lat_rows, waves, sections)

    block_m = waves // groups
    block_n = waves // sections
    deal = total.shape[1] // groups
    outgoing = total.reshape(sections, mine, groups, deal, LANES)
    outgoing = outgoing.transpose(2, 0, 1, 3, 4).reshape(groups * sections, mine * deal, LANES)
    arrived = lax.all_to_all(outgoing, ("lev", "tm"), split_axis=0, concat_axis=0, tiled=True)
    arrived = arrived.reshape(groups, padded, deal * LANES)[:, :lev_dev].reshape(levels, deal * LANES)
    result = jnp.einsum("kj,kx->jx", vertical, arrived, precision=PRECISE)
    return result.reshape(levels, block_m, 2, block_n)


def solution(mesh):
    placed = (
        P("tm", None),
        P("tm", "lev", None),
        P("tm", "lev", None, None),
        P("tm", None, None),
        P(),
        P(),
    )
    return jax.shard_map(
        shards, mesh=mesh, in_specs=placed, out_specs=P(None, "lev", None, "tm"), check_vma=False
    )
```

```python
import functools
import math

import jax
import jax.numpy as jnp
import numpy as np
from jax import lax
from jax.experimental import pallas as pl
from jax.experimental.pallas import tpu as pltpu
from jax.sharding import PartitionSpec as P

PRECISE = lax.Precision.HIGHEST
BF16 = jnp.bfloat16
F32 = jnp.float32
NT = (((1,), (1,)), ((), ()))
NN = (((1,), (0,)), ((), ()))
VMEM_BYTES = 62 * 1024 * 1024
LANES = 128
SUBLANES = 8


def dot(left, right, dims):
    return lax.dot_general(left, right, dims, preferred_element_type=F32)


def halves(value):
    high = value.astype(BF16)
    return high, (value - high.astype(F32)).astype(BF16)


def fourier_rows(lon_count, wave_count):
    index = np.arange(wave_count)[:, None] * np.arange(lon_count)[None, :] % lon_count
    angles = 2.0 * np.pi * index / lon_count
    return (np.concatenate([np.cos(angles), np.sin(angles)], 0) * np.sqrt(2.0 / lon_count)).astype(np.float32)


def legendre_coefficients(lat_count, wave_count):
    half = lat_count // 2
    pack = 2 * LANES // half
    groups = wave_count // pack
    deep = LANES // pack
    phi = (np.arange(half) + 0.5) * np.pi / lat_count - 0.5 * np.pi
    orders = np.arange(wave_count).astype(np.float64)
    lead = np.array(
        [
            -0.5 * math.log(2.0)
            + 0.5 * (math.lgamma(m + 1.5) - math.lgamma(1.5) - math.lgamma(m + 1.0))
            for m in range(wave_count)
        ]
    )
    weight = np.sqrt(np.pi * np.cos(phi) / lat_count)
    diagonal = weight[None, :] * np.exp(lead[:, None] + orders[:, None] * np.log(np.cos(phi))[None, :])
    diagonal = diagonal.reshape(groups, pack * half)
    mu = np.broadcast_to(np.tile(np.sin(phi), pack)[None, :], (groups, pack * half))
    degree = orders[:, None]
    above = degree > orders[None, :]
    gap = np.where(above, degree**2 - orders[None, :] ** 2, 1.0)
    up = np.where(above, np.sqrt(np.maximum(4.0 * degree**2 - 1.0, 0.0) / gap), 0.0)
    lower = degree - 1.0
    down = np.sqrt(np.maximum(lower**2 - orders[None, :] ** 2, 0.0) / np.maximum(4.0 * lower**2 - 1.0, 1.0))

    def packed(a):
        a = a.reshape(wave_count // deep, deep, groups, pack)
        return a.transpose(0, 2, 1, 3).reshape(wave_count // deep * groups, deep * pack)

    return [np.asarray(a, np.float32) for a in (mu, diagonal, packed(up), packed(up * down))]


def meet(axis):
    count = lax.axis_size(axis)
    me = lax.axis_index(axis)
    barrier = pltpu.get_barrier_semaphore()
    for d in range(1, count):
        pl.semaphore_signal(
            barrier, inc=1, device_id={axis: lax.rem(me + d, count)}, device_id_type=pl.DeviceIdType.MESH
        )
    pl.semaphore_wait(barrier, count - 1)


def rates_for(tangent_ref, rows, section):
    start = jnp.minimum(section * rows, tangent_ref.shape[0] - rows)
    return tangent_ref.at[pl.ds(pl.multiple_of(start, SUBLANES), rows), :]


def rate_copies(source, tangent_ref, place, sent, landed):
    sections = lax.axis_size("tm")
    copies = []
    for d in range(1, sections):
        peer = lax.rem(jnp.int32(source + d), sections)
        copies.append(
            pltpu.make_async_remote_copy(
                src_ref=rates_for(tangent_ref, place.shape[0], peer),
                dst_ref=place,
                send_sem=sent.at[d],
                recv_sem=landed,
                device_id={"tm": peer},
                device_id_type=pl.DeviceIdType.MESH,
            )
        )
    return copies


def bin_shape(lat_rows, lon_cols):
    tall = math.gcd(lat_rows, 32)
    return tall, (lat_rows // tall) * (lon_cols // LANES)


def sort_kernel(
    lon_cols, tall, bins, mine, cell_ref, innov_ref, damp_ref, tangent_ref, out_ref, rate_ref,
    lane_from, sub_from, swaps, sent, landed,
):
    levels, deep, _ = innov_ref.shape
    sections = out_ref.shape[0]
    me = lax.axis_index("tm")
    meet("tm")
    copies = rate_copies(sections - 1, tangent_ref, rate_ref, sent, landed)

    @pl.when(me == sections - 1)
    def _():
        for copy in copies:
            copy.start()

    blocks = deep // SUBLANES
    low_bits, mid_bits, top_bits = (n.bit_length() - 1 for n in (blocks, SUBLANES, LANES))
    mid_end = low_bits + mid_bits
    all_bits = mid_end + top_bits
    lane = lax.broadcasted_iota(jnp.int32, (SUBLANES, LANES), 1)
    sub = lax.broadcasted_iota(jnp.int32, (SUBLANES, LANES), 0)
    span = tall * LANES
    wide = lon_cols // LANES

    def key_of(cells):
        rows = cells // lon_cols
        cols = cells - rows * lon_cols
        tile = (rows // tall) * wide + cols // LANES
        return tile * span + (rows % tall) * LANES + cols % LANES

    keys = [key_of(cell_ref[v * SUBLANES : (v + 1) * SUBLANES, :]) for v in range(blocks)]

    def falling(stage):
        if stage >= all_bits:
            return None
        if stage >= mid_end:
            return (lane >> (stage - mid_end)) & 1
        return (sub >> (stage - low_bits)) & 1

    plan = []

    def across(values, bits, position, axis, stage, first, last):
        down = falling(stage)
        values = [value * (1 << bits) + position for value in values]
        for bit in range(first, last - 1, -1):
            reach = 1 << bit
            index = position ^ reach
            upper = (position >> bit) & 1
            keep = (upper if down is None else upper ^ down) == 0
            moved = []
            for value in values:
                other = jnp.take_along_axis(value, index, axis=axis, mode="promise_in_bounds")
                moved.append(jnp.where(keep, jnp.minimum(value, other), jnp.maximum(value, other)))
            values = moved
        return [value >> bits for value in values], [value & ((1 << bits) - 1) for value in values]

    for stage in range(1, all_bits + 1):
        if stage > mid_end:
            keys, source = across(keys, top_bits, lane, 1, stage, stage - 1 - mid_end, 0)
            slot = sum(1 for kind, _ in plan if kind == "lane")
            for v in range(blocks):
                lane_from[slot, v] = source[v]
            plan.append(("lane", slot))
        if stage > low_bits:
            keys, source = across(keys, mid_bits, sub, 0, stage, min(stage, mid_end) - 1 - low_bits, 0)
            slot = sum(1 for kind, _ in plan if kind == "sub")
            for v in range(blocks):
                sub_from[slot, v] = source[v]
            plan.append(("sub", slot))
        for bit in range(min(stage, low_bits) - 1, -1, -1):
            down = None if stage < low_bits else falling(stage)
            slot = sum(1 for kind, _ in plan if kind == "swap")
            pair = 0
            for v in range(blocks):
                if v >> bit & 1:
                    continue
                first, second = keys[v], keys[v | 1 << bit]
                if stage < low_bits:
                    swap = first < second if v >> stage & 1 else first > second
                elif down is None:
                    swap = first > second
                else:
                    swap = jnp.where(down == 0, first - second, second - first) > 0
                swaps[slot, pair] = jnp.where(swap, 1, 0)
                keys[v], keys[v | 1 << bit] = jnp.where(swap, second, first), jnp.where(swap, first, second)
                pair += 1
            plan.append(("swap", (slot, bit)))

    for s in range(sections):
        out_ref[s, mine * deep : (mine + 1) * deep, :] = jnp.concatenate([key.astype(F32) for key in keys], 0).T

    edges = jnp.zeros((1, LANES), F32)
    for b in range(1, bins + 1):
        below = sum(jnp.where(key < b * span, 1.0, 0.0) for key in keys)
        below = jnp.sum(jnp.sum(below, 0, keepdims=True), 1, keepdims=True)
        edges = jnp.where(lane[:1] == b, below, edges)
    extra = mine * damp_ref.shape[1] // LANES
    first = lax.axis_index("lev") * levels
    base = (mine + 1) * deep
    for s in range(sections):
        place = jnp.minimum(first + s * mine, damp_ref.shape[0] - mine)
        rows = [damp_ref[pl.ds(place + k, 1), :] for k in range(mine)]
        tail = rows + [edges, jnp.zeros((SUBLANES - extra - 1, LANES), F32)]
        out_ref[s, base : base + SUBLANES, :] = jnp.concatenate(tail, 0)
        for k in range(mine):
            if s * mine + k >= levels:
                out_ref[s, k * deep : (k + 1) * deep, :] = jnp.zeros((deep, LANES), F32)

    def move(p, carry):
        values = [innov_ref[p, v * SUBLANES : (v + 1) * SUBLANES, :] for v in range(blocks)]
        for kind, slot in plan:
            if kind == "swap":
                slot, bit = slot
                firsts = [v for v in range(blocks) if not v >> bit & 1]
                for pair, v in enumerate(firsts):
                    swap = swaps[slot, pair] != 0
                    first, second = values[v], values[v | 1 << bit]
                    values[v] = jnp.where(swap, second, first)
                    values[v | 1 << bit] = jnp.where(swap, first, second)
            else:
                ref, axis = (lane_from, 1) if kind == "lane" else (sub_from, 0)
                values = [
                    jnp.take_along_axis(value, ref[slot, v], axis=axis, mode="promise_in_bounds")
                    for v, value in enumerate(values)
                ]
        out_ref[p // mine, pl.ds(pl.multiple_of(p % mine * deep, deep), deep), :] = jnp.concatenate(values, 0).T
        return carry

    lax.fori_loop(0, levels, move, 0)

    @pl.when(me == sections - 1)
    def _():
        for copy in copies:
            copy.wait_send()

    @pl.when(me != sections - 1)
    def _():
        copies[0].wait_recv()


def sorted_message(cells, innov, damp, tangent, sections, mine, lat_rows, lon_cols):
    levels, deep, _ = innov.shape
    blocks = deep // SUBLANES
    low_bits, mid_bits, top_bits = (n.bit_length() - 1 for n in (blocks, SUBLANES, LANES))
    all_bits = low_bits + mid_bits + top_bits
    tall, bins = bin_shape(lat_rows, lon_cols)
    swap_count = sum(min(stage, low_bits) for stage in range(1, all_bits + 1))
    return pl.pallas_call(
        functools.partial(sort_kernel, lon_cols, tall, bins, mine),
        in_specs=[pl.BlockSpec(memory_space=pltpu.VMEM)] * 3 + [pl.BlockSpec(memory_space=pl.ANY)],
        out_specs=[pl.BlockSpec(memory_space=pltpu.VMEM), pl.BlockSpec(memory_space=pl.ANY)],
        out_shape=[
            jax.ShapeDtypeStruct((sections, (mine + 1) * deep + SUBLANES, LANES), F32),
            jax.ShapeDtypeStruct((mine * lat_rows, lon_cols), F32),
        ],
        scratch_shapes=[
            pltpu.VMEM((top_bits, blocks, SUBLANES, LANES), jnp.int32),
            pltpu.VMEM((top_bits + mid_bits, blocks, SUBLANES, LANES), jnp.int32),
            pltpu.VMEM((swap_count, max(1, blocks // 2), SUBLANES, LANES), jnp.int32),
            pltpu.SemaphoreType.DMA((sections,)),
            pltpu.SemaphoreType.DMA,
        ],
        compiler_params=pltpu.CompilerParams(
            collective_id=2, has_side_effects=True, vmem_limit_bytes=10 * 2**20
        ),
        cost_estimate=pl.CostEstimate(flops=2**30, bytes_accessed=2**21, transcendentals=0),
    )(cells, innov, damp, tangent)


def forcing_kernel(
    mine, extra, tall, message_ref, tangent_ref, out_ref, rate_ref, run_ref, edge_ref, edge_sem, sent, landed,
):
    times = message_ref.shape[0]
    bins = out_ref.shape[1]
    me = lax.axis_index("tm")
    meet("tm")
    traffic = [rate_copies(t, tangent_ref, rate_ref.at[t - 1], sent, landed.at[t]) for t in range(1, times - 1)]
    for t, copies in enumerate(traffic, 1):

        @pl.when(me == t)
        def _():
            for copy in copies:
                copy.start()

    deep = (message_ref.shape[1] - SUBLANES) // (mine + 1)
    chunks = deep // 2
    span = tall * LANES
    load = pltpu.make_async_copy(message_ref.at[:, (mine + 1) * deep + extra, :], edge_ref, edge_sem)
    load.start()
    run_ref[:, 0] = jnp.zeros(run_ref.shape[:1] + run_ref.shape[2:], F32)
    col_ids = lax.broadcasted_iota(jnp.int32, (LANES, 2 * LANES), 0).astype(F32).astype(BF16)
    row_ids = lax.broadcasted_iota(jnp.int32, (tall, 2 * LANES), 0).astype(F32).astype(BF16)
    one, none = jnp.ones((), BF16), jnp.zeros((), BF16)

    def row_of(t, base, c):
        return jnp.concatenate([message_ref[t, pl.ds(base + 2 * c + i, 1), :] for i in range(2)], 1)

    def visit(t, b, c, live):
        key = row_of(t, mine * deep, c).astype(jnp.int32) - jnp.where(live, b, bins + 1) * span
        cols = (key & (LANES - 1)).astype(F32).astype(BF16)
        rows = (key >> 7).astype(F32).astype(BF16)
        spread_cols = jnp.where(col_ids == jnp.broadcast_to(cols, col_ids.shape), one, none)
        hit = row_ids == jnp.broadcast_to(rows, row_ids.shape)
        parts = [halves(row_of(t, k * deep, c)) for k in range(mine)]
        pieces = [jnp.where(hit, jnp.broadcast_to(part[i], row_ids.shape), none) for i in range(2) for part in parts]
        field = dot(jnp.concatenate(pieces, 0), spread_cols, NT)
        return field[: mine * tall] + field[mine * tall :]

    total = chunks + bins - 1
    unroll = 4
    load.wait()

    def walk(s, state):
        fields, nexts = [], []
        for t in range(times):
            b, c, same = state[t]
            for u in range(unroll):
                place = s * unroll + u
                fields.append((t, place, same, visit(t, b, c, place < total)))
                stay = (edge_ref[t, b + 1].astype(jnp.int32) > (c + 1) * 2 * LANES).astype(jnp.int32)
                after = jnp.minimum(b + 1 - stay, bins - 1)
                same = (after == b).astype(F32)
                b, c = after, jnp.minimum(c + stay, chunks - 1)
            nexts.append((b, c, same))
        for t, place, same, field in fields:
            run_ref[t, place + 1] = run_ref[t, place] * same + field
        return tuple(nexts)

    start = jnp.int32(0)
    steps = -(-total // unroll)
    lax.fori_loop(0, steps, walk, tuple((start, start, jnp.float32(0)) for _ in range(times)))

    def place_bin(b, carry):
        for t in range(times):
            end = edge_ref[t, b + 1].astype(jnp.int32)
            last = b + jnp.maximum((end + 2 * LANES - 1) // (2 * LANES) - 1, 0)
            last = jnp.where(b == bins - 1, steps * unroll - 1, last)
            last = jnp.minimum(jnp.maximum(last, 0), steps * unroll - 1)
            out_ref[t, b] = run_ref[t, last + 1]
        return carry

    lax.fori_loop(0, bins, place_bin, 0)
    for t, copies in enumerate(traffic, 1):

        @pl.when(me == t)
        def _():
            for copy in copies:
                copy.wait_send()

        @pl.when(me != t)
        def _():
            copies[0].wait_recv()


def forcing_fields(message, tangent, mine, extra, lat_rows, lon_cols):
    times = message.shape[0]
    tall, bins = bin_shape(lat_rows, lon_cols)
    deep = (message.shape[1] - SUBLANES) // (mine + 1)
    places = -(-(deep // 2 + bins - 1) // 4) * 4 + 1
    return pl.pallas_call(
        functools.partial(forcing_kernel, mine, extra, tall),
        in_specs=[pl.BlockSpec(memory_space=pltpu.VMEM), pl.BlockSpec(memory_space=pl.ANY)],
        out_specs=[pl.BlockSpec(memory_space=pltpu.VMEM), pl.BlockSpec(memory_space=pl.ANY)],
        out_shape=[
            jax.ShapeDtypeStruct((times, bins, mine * tall, LANES), F32),
            jax.ShapeDtypeStruct((times - 2, mine * lat_rows, lon_cols), F32),
        ],
        scratch_shapes=[
            pltpu.VMEM((times, places, mine * tall, LANES), F32),
            pltpu.SMEM((times, LANES), F32),
            pltpu.SemaphoreType.DMA,
            pltpu.SemaphoreType.DMA((times,)),
            pltpu.SemaphoreType.DMA((times,)),
        ],
        compiler_params=pltpu.CompilerParams(
            collective_id=3, has_side_effects=True, vmem_limit_bytes=4 * times * places * mine * tall * LANES + 10 * 2**20
        ),
        cost_estimate=pl.CostEstimate(flops=2**33, bytes_accessed=2**22, transcendentals=0),
    )(message, tangent)


def lanes_at(value, index):
    return jnp.take_along_axis(value, jnp.broadcast_to(index, value.shape), axis=1, mode="promise_in_bounds")


def legendre_tables(half, mu_ref, diag_ref, up_ref, both_ref, high, low, left, right):
    groups, width = mu_ref.shape
    waves = high.shape[1]
    pack = width // half
    deep = LANES // pack
    lane = lax.broadcasted_iota(jnp.int32, (1, LANES), 1)
    sub = lax.broadcasted_iota(jnp.int32, (groups, width), 0)
    orders = sub * pack + lax.broadcasted_iota(jnp.int32, (groups, width), 1) // half

    def advance(n, state):
        one, two = state
        place = pl.ds(pl.multiple_of(n // deep * groups, groups), groups)
        base = (n % deep) * pack

        def spread_out(ref):
            value = ref[place, :]
            return jnp.concatenate([lanes_at(value, base + lane // half + i * (LANES // half)) for i in range(width // LANES)], 1)

        recurred = spread_out(up_ref) * (mu_ref[...] * one) - spread_out(both_ref) * two
        value = jnp.where(orders == n, diag_ref[...], recurred)
        row = (n % 2) * (waves // 2) + n // 2
        left[pl.ds(row, groups, stride=waves), :] = value[:, :LANES]
        right[pl.ds(row, groups, stride=waves), :] = value[:, LANES:]
        return value, one

    zero = 0.0 * mu_ref[...]
    lax.fori_loop(0, waves, advance, (zero, zero), unroll=8)

    def split(g, carry):
        for i, ref in enumerate((left, right)):
            upper, lower = halves(ref[pl.ds(pl.multiple_of(g * waves, waves), waves), :])
            high[g, :, i * LANES : (i + 1) * LANES] = upper
            low[g, :, i * LANES : (i + 1) * LANES] = lower
        return carry

    lax.fori_loop(0, groups, split, 0, unroll=4)


def exchange_kernel(
    half, message_ref, mu_ref, diag_ref, up_ref, both_ref, out_ref, high_ref, low_ref,
    high, low, left, right, sent, landed, own, stored,
):
    sections = lax.axis_size("tm")
    me = lax.axis_index("tm")
    meet("tm")
    copies = []
    for d in range(1, sections):
        peer = lax.rem(me + d, sections)
        copies.append(
            pltpu.make_async_remote_copy(
                src_ref=message_ref.at[peer],
                dst_ref=out_ref.at[me],
                send_sem=sent.at[d],
                recv_sem=landed.at[d],
                device_id={"tm": peer},
                device_id_type=pl.DeviceIdType.MESH,
            )
        )
        copies[-1].start()
    keep = pltpu.make_async_copy(message_ref.at[me], out_ref.at[me], own)
    keep.start()
    legendre_tables(half, mu_ref, diag_ref, up_ref, both_ref, high, low, left, right)
    saves = [
        pltpu.make_async_copy(high, high_ref, stored.at[0]),
        pltpu.make_async_copy(low, low_ref, stored.at[1]),
    ]
    for save in saves:
        save.start()
    keep.wait()
    for save in saves:
        save.wait()
    for copy in copies:
        copy.wait()


def exchanged(message, lat_rows, waves):
    mu, diagonal, up, both = legendre_coefficients(lat_rows, waves)
    groups, width = mu.shape
    sections = message.shape[0]
    table = jax.ShapeDtypeStruct((groups, waves, width), BF16)
    vmem = pl.BlockSpec(memory_space=pltpu.VMEM)
    return pl.pallas_call(
        functools.partial(exchange_kernel, lat_rows // 2),
        in_specs=[vmem] * 5,
        out_specs=[vmem, pl.BlockSpec(memory_space=pl.ANY), pl.BlockSpec(memory_space=pl.ANY)],
        out_shape=[jax.ShapeDtypeStruct(message.shape, F32), table, table],
        scratch_shapes=[
            pltpu.VMEM((groups, waves, width), BF16),
            pltpu.VMEM((groups, waves, width), BF16),
            pltpu.VMEM((waves * groups, LANES), F32),
            pltpu.VMEM((waves * groups, LANES), F32),
            pltpu.SemaphoreType.DMA((sections,)),
            pltpu.SemaphoreType.DMA((sections,)),
            pltpu.SemaphoreType.DMA,
            pltpu.SemaphoreType.DMA((2,)),
        ],
        compiler_params=pltpu.CompilerParams(
            collective_id=0, has_side_effects=True, vmem_limit_bytes=16 * 2**20
        ),
        cost_estimate=pl.CostEstimate(flops=2**32, bytes_accessed=2**23, transcendentals=0),
    )(message, mu, diagonal, up, both)


def gather_kernel(total_ref, out_ref, sent, landed, own):
    sections, groups = lax.axis_size("tm"), lax.axis_size("lev")
    count = sections * groups
    me = lax.axis_index("lev") * sections + lax.axis_index("tm")

    def place(index):
        return {"tm": lax.rem(index, sections), "lev": lax.div(index, sections)}

    barrier = pltpu.get_barrier_semaphore()

    def greet(d, carry):
        pl.semaphore_signal(
            barrier, inc=1, device_id=place(lax.rem(me + d, count)), device_id_type=pl.DeviceIdType.MESH
        )
        return carry

    lax.fori_loop(1, count, greet, 0)
    keep = pltpu.make_async_copy(total_ref.at[me], out_ref.at[me], own)
    keep.start()
    pl.semaphore_wait(barrier, count - 1)

    def copy_to(d):
        peer = lax.rem(me + d, count)
        return pltpu.make_async_remote_copy(
            src_ref=total_ref.at[peer],
            dst_ref=out_ref.at[me],
            send_sem=sent.at[d],
            recv_sem=landed.at[d],
            device_id=place(peer),
            device_id_type=pl.DeviceIdType.MESH,
        )

    def send(d, carry):
        copy_to(d).start()
        return carry

    def finish(d, carry):
        copy_to(d).wait()
        return carry

    lax.fori_loop(1, count, send, 0)
    keep.wait()
    lax.fori_loop(1, count, finish, 0)


def gathered(total):
    count = total.shape[0]
    vmem = pl.BlockSpec(memory_space=pltpu.VMEM)
    return pl.pallas_call(
        gather_kernel,
        in_specs=[vmem],
        out_specs=vmem,
        out_shape=jax.ShapeDtypeStruct(total.shape, F32),
        scratch_shapes=[
            pltpu.SemaphoreType.DMA((count,)),
            pltpu.SemaphoreType.DMA((count,)),
            pltpu.SemaphoreType.DMA,
        ],
        compiler_params=pltpu.CompilerParams(collective_id=1, has_side_effects=True, vmem_limit_bytes=4 * 2**20),
        cost_estimate=pl.CostEstimate(flops=2**30, bytes_accessed=2**20, transcendentals=0),
    )(total)


def sweep_kernel(
    base, field_hbm, own_hbm, rate_hbm, later_hbm, message_hbm, spread_ref, fhigh_ref, flow_ref, high_hbm, low_hbm,
    out_ref, field_ref, tangent_ref, tail_ref, high, low, even, odd, packed, total, adjoint, order,
    field_sem, tangent_sem, tail_sem, table_sem,
):
    times, rows, lon_cols = tangent_ref.shape
    sections = lax.axis_size("tm")
    load_tail = pltpu.make_async_copy(message_hbm.at[:, pl.ds(base, SUBLANES), :], tail_ref, tail_sem)
    load_tables = [
        pltpu.make_async_copy(high_hbm, high, table_sem.at[0]),
        pltpu.make_async_copy(low_hbm, low, table_sem.at[1]),
    ]

    def load_field(t):
        return pltpu.make_async_copy(field_hbm.at[t], field_ref.at[t], field_sem.at[t])

    me = lax.axis_index("tm")
    own = rates_for(own_hbm, rows, me)

    def load_tangent(t):
        return pltpu.make_async_copy(own, tangent_ref.at[t], tangent_sem.at[t])

    def start_tangent(t):
        @pl.when(me == t)
        def _():
            load_tangent(t).start()

        @pl.when(me != t)
        def _():
            source = rate_hbm if t == times - 1 else later_hbm.at[t - 1]
            pltpu.make_async_copy(source, tangent_ref.at[t], tangent_sem.at[t]).start()

    load_field(times - 1).start()
    load_tail.start()
    for load in load_tables:
        load.start()
    start_tangent(times - 1)
    for t in range(times - 2, -1, -1):
        load_field(t).start()
        if t > 0:
            start_tangent(t)
    bins = field_ref.shape[1]
    groups, waves, width = high.shape
    lat_rows = width * groups * 2 // waves
    half = lat_rows // 2
    pack = width // half
    deep = LANES // pack
    levels = rows // lat_rows
    tall = field_ref.shape[2] // levels
    across = lon_cols // LANES
    group = 4 * levels
    mid = group // 2

    lane = lax.broadcasted_iota(jnp.int32, (1, LANES), 1)
    in_first = lane < half
    fold = lane % half
    in_high = lax.broadcasted_iota(jnp.int32, (group, LANES), 0) < mid
    n_even = lax.broadcasted_iota(jnp.int32, (group, LANES), 1) < waves // 2
    lat_south = lax.broadcasted_iota(jnp.int32, (group, LANES), 1) < half
    adjoint[...] = jnp.zeros_like(adjoint)
    total[...] = jnp.zeros_like(total)
    own_half = (lax.broadcasted_iota(jnp.int32, (waves, LANES), 1) // half) == (
        lax.broadcasted_iota(jnp.int32, (waves, LANES), 0) % (LANES // half)
    )

    load_tail.wait()

    def damp_of(t):
        index = 2 * (lane % (waves // 2)) + lane // (waves // 2)
        row = lax.broadcasted_iota(jnp.int32, (group, LANES), 0) % mid // 2
        value = jnp.zeros((group, LANES), F32)
        for k in range(levels):
            value = jnp.where(row == k, jnp.broadcast_to(tail_ref[t, k : k + 1, :], value.shape), value)
        return lanes_at(value, index)

    def analyse(t):
        load_field(t).wait()
        field = [
            jnp.concatenate([field_ref[t, h + i, k * tall : (k + 1) * tall, :] for i in range(across)], 1)
            for k in range(levels)
            for h in range(0, bins, across)
        ]
        forced = adjoint[...] + jnp.concatenate(field, 0)
        adjoint[...] = forced
        upper, lower = halves(forced)
        coeffs = dot(fhigh_ref[...], upper, NT) + dot(flow_ref[...], upper, NT) + dot(fhigh_ref[...], lower, NT)
        for k in range(levels):
            for p in range(2):
                part = coeffs[p * waves : (p + 1) * waves, k * lat_rows : (k + 1) * lat_rows]
                south = lanes_at(part, fold)
                north = lanes_at(part, lat_rows - 1 - fold)
                for value, ref in ((south + north, even), (south - north, odd)):
                    value = jnp.where(own_half, value, 0.0)
                    rounded = value.astype(BF16).astype(F32)
                    ref[pl.ds(2 * k + p, waves, stride=group), :] = rounded
                    ref[pl.ds(mid + 2 * k + p, waves, stride=group), :] = value - rounded

    def pair_sum(value):
        return value + pltpu.roll(value, mid, 0)

    blank = jnp.zeros((group, LANES), F32)
    per_tile = LANES // half

    def place_of(g, i):
        return pl.ds(pl.multiple_of((g * pack + i) * group, group), group)

    def spectral_of(g):
        lefts = []
        for i in range(pack):
            for ref in (even, odd):
                value = ref[place_of(g, i), :]
                tiles = [value if i // per_tile == c else blank for c in range(width // LANES)]
                lefts.append(jnp.concatenate(tiles, 1))
        lefts = jnp.concatenate(lefts, 0).astype(BF16)
        product = dot(lefts, high[g], NT) + dot(lefts, low[g], NT)
        values = []
        for i in range(pack):
            same = product[2 * i * group : (2 * i + 1) * group]
            other = product[(2 * i + 1) * group : (2 * i + 2) * group]
            value = pair_sum(jnp.where(n_even, same, other) if i % 2 == 0 else jnp.where(n_even, other, same))
            total[place_of(g, i), :] += value
            values.append(value)
        return values

    def synthesise(g, values, damp):
        lefts = []
        for i, value in enumerate(values):
            filtered = value * damp
            rounded = filtered.astype(BF16).astype(F32)
            parts = jnp.where(in_high, rounded, filtered - rounded)
            first, second = jnp.where(n_even, parts, 0.0), jnp.where(n_even, 0.0, parts)
            lefts += [first, second] if i % 2 == 0 else [second, first]
        lefts = jnp.concatenate(lefts, 0).astype(BF16)
        product = dot(lefts, high[g], NN) + dot(lefts, low[g], NN)
        for i in range(pack):
            tile = slice(i // per_tile * LANES, (i // per_tile + 1) * LANES)
            same = product[2 * i * group : (2 * i + 1) * group, tile]
            other = product[(2 * i + 1) * group : (2 * i + 2) * group, tile]
            index = (i % per_tile) * half + jnp.where(in_first, lane, lat_rows - 1 - lane)
            same, other = lanes_at(same, index), lanes_at(other, index)
            packed[place_of(g, i), :] = pair_sum(jnp.where(lat_south, same + other, same - other))

    def step(s, carry):
        t = times - 1 - s
        analyse(t)
        damp = damp_of(t)

        @pl.when(s == 0)
        def _():
            for load in load_tables:
                load.wait()

        def wave(g, inner):
            for i, value in enumerate(spectral_of(g)):
                packed[place_of(g, i), :] = value
            return inner

        def back(g, inner):
            synthesise(g, [packed[place_of(g, i), :] for i in range(pack)], damp)
            return inner

        lax.fori_loop(0, groups, wave, 0, unroll=32)
        lax.fori_loop(0, groups, back, 0, unroll=32)
        synth = jnp.concatenate(
            [
                jnp.concatenate([packed[pl.ds(2 * k + p, waves, stride=group), :] for p in range(2)], 0).T
                for k in range(levels)
            ],
            0,
        )
        upper, lower = halves(synth)
        gridded = dot(upper, fhigh_ref[...], NN) + dot(lower, fhigh_ref[...], NN) + dot(upper, flow_ref[...], NN)
        load_tangent(t).wait()
        adjoint[...] = tangent_ref[t] * adjoint[...] + gridded
        return carry

    lax.fori_loop(0, times - 1, step, 0)
    analyse(0)

    def last(g, inner):
        spectral_of(g)
        return inner

    lax.fori_loop(0, groups, last, 0, unroll=32)

    block_n = waves // sections
    side = LANES // block_n
    deal = 2 * waves // side
    natural = (lane % 2) * (waves // 2) + lane // 2
    lev_dev = spread_ref.shape[0] // lax.axis_size("lev")
    first = lax.axis_index("lev") * lev_dev + lax.axis_index("tm") * levels
    first = jnp.minimum(first, spread_ref.shape[0] - levels)
    for k in range(levels):
        for p in range(2):
            value = total[pl.ds(2 * k + p, waves, stride=group), :]
            order[pl.ds(p, waves, stride=2), :] = lanes_at(value, natural) * spread_ref[pl.ds(first + k, 1), :]
        blocks = [order[pl.ds(q, deal, stride=side), :] for q in range(side)]
        for s in range(sections):
            value = blocks[0] if s == 0 else pltpu.roll(blocks[0], (-s * block_n) % LANES, 1)
            for q in range(1, side):
                moved = blocks[q] if q == s else pltpu.roll(blocks[q], ((q - s) * block_n) % LANES, 1)
                value = jnp.where(lane // block_n == q, moved, value)
            rows = deal * sections // out_ref.shape[0]
            for b in range(out_ref.shape[0] // sections):
                out_ref[b * sections + s, k * rows : (k + 1) * rows, :] = value[b * rows : (b + 1) * rows]


def sweep(fields, tangent, rate, later, message, spread, high, low, lat_rows, base, sections, blocks):
    times = fields.shape[0]
    rows, lon_cols = rate.shape
    levels = rows // lat_rows
    group = 4 * levels
    groups, waves, width = high.shape
    fourier = fourier_rows(lon_cols, waves)
    fhigh = fourier.astype(jnp.bfloat16)
    flow = (fourier - fhigh.astype(np.float32)).astype(jnp.bfloat16)
    deal = 2 * waves * (waves // sections) // LANES // blocks
    vmem, hbm = pl.BlockSpec(memory_space=pltpu.VMEM), pl.BlockSpec(memory_space=pl.ANY)
    return pl.pallas_call(
        functools.partial(sweep_kernel, base),
        in_specs=[hbm, hbm, hbm, hbm, hbm, vmem, vmem, vmem, hbm, hbm],
        out_specs=vmem,
        out_shape=jax.ShapeDtypeStruct((blocks * sections, levels * deal, LANES), F32),
        scratch_shapes=[
            pltpu.VMEM(fields.shape, F32),
            pltpu.VMEM((times, rows, lon_cols), F32),
            pltpu.VMEM((times, SUBLANES, LANES), F32),
            pltpu.VMEM((groups, waves, width), BF16),
            pltpu.VMEM((groups, waves, width), BF16),
            pltpu.VMEM((waves * group, LANES), F32),
            pltpu.VMEM((waves * group, LANES), F32),
            pltpu.VMEM((waves * group, LANES), F32),
            pltpu.VMEM((waves * group, LANES), F32),
            pltpu.VMEM((rows, lon_cols), F32),
            pltpu.VMEM((2 * waves, LANES), F32),
            pltpu.SemaphoreType.DMA((times,)),
            pltpu.SemaphoreType.DMA((times,)),
            pltpu.SemaphoreType.DMA,
            pltpu.SemaphoreType.DMA((2,)),
        ],
        compiler_params=pltpu.CompilerParams(vmem_limit_bytes=24 * 2**20),
        cost_estimate=pl.CostEstimate(flops=2**34, bytes_accessed=2**22, transcendentals=0),
    )(fields, tangent, rate, later, message, spread, fhigh, flow, high, low)


def shards(obs_cell, innovation, tangent, damping, spread, vertical):
    sections = lax.axis_size("tm")
    groups = lax.axis_size("lev")
    lev_dev, lat_rows, lon_cols = tangent.shape[1:]
    levels, waves = damping.shape[1:]
    mine = -(-lev_dev // sections)
    mine += mine % 2
    padded = mine * sections

    def pad_levels(value, axis):
        widths = [(0, 0)] * value.ndim
        widths[axis] = (0, padded - value.shape[axis])
        return jnp.pad(value, widths) if padded > value.shape[axis] else value

    count = obs_cell.shape[1]
    deep = count // LANES
    message, rate = sorted_message(
        obs_cell.reshape(deep, LANES),
        innovation.reshape(lev_dev, deep, LANES),
        damping[0],
        tangent.reshape(lev_dev * lat_rows, lon_cols),
        sections,
        mine,
        lat_rows,
        lon_cols,
    )
    message, high, low = exchanged(message, lat_rows, waves)
    base = (mine + 1) * deep
    rates = tangent.reshape(lev_dev * lat_rows, lon_cols)
    fields, later = forcing_fields(message, rates, mine, mine * waves // LANES, lat_rows, lon_cols)
    total = sweep(fields, rates, rate, later, message, spread, high, low, lat_rows, base, sections, groups)

    block_m = waves // groups
    block_n = waves // sections
    deal = total.shape[1] // mine
    arrived = gathered(total).reshape(groups, padded, deal * LANES)[:, :lev_dev].reshape(levels, deal * LANES)
    result = jnp.einsum("kj,kx->jx", vertical, arrived, precision=PRECISE)
    return result.reshape(levels, block_m, 2, block_n)


def solution(mesh):
    placed = (
        P("tm", None),
        P("tm", "lev", None),
        P("tm", "lev", None, None),
        P("tm", None, None),
        P(),
        P(),
    )
    return jax.shard_map(
        shards, mesh=mesh, in_specs=placed, out_specs=P(None, "lev", None, "tm"), check_vma=False
    )
```

```python
import functools
import math

import jax
import jax.numpy as jnp
import numpy as np
from jax import lax
from jax.experimental import pallas as pl
from jax.experimental.pallas import tpu as pltpu
from jax.sharding import PartitionSpec as P

PRECISE = lax.Precision.HIGHEST
BF16 = jnp.bfloat16
F32 = jnp.float32
NT = (((1,), (1,)), ((), ()))
NN = (((1,), (0,)), ((), ()))
VMEM_BYTES = 67043328
LANES = 128
SUBLANES = 8


def dot(left, right, dims):
    return lax.dot_general(left, right, dims, preferred_element_type=F32)


def halves(value):
    high = value.astype(BF16)
    return high, (value - high.astype(F32)).astype(BF16)


def fourier_rows(lon_count, wave_count):
    index = np.arange(wave_count)[:, None] * np.arange(lon_count)[None, :] % lon_count
    angles = 2.0 * np.pi * index / lon_count
    return (np.concatenate([np.cos(angles), np.sin(angles)], 0) * np.sqrt(2.0 / lon_count)).astype(np.float32)


def legendre_coefficients(lat_count, wave_count):
    half = lat_count // 2
    pack = 2 * LANES // half
    groups = wave_count // pack
    deep = LANES // pack
    phi = (np.arange(half) + 0.5) * np.pi / lat_count - 0.5 * np.pi
    orders = np.arange(wave_count).astype(np.float64)
    lead = np.array(
        [
            -0.5 * math.log(2.0)
            + 0.5 * (math.lgamma(m + 1.5) - math.lgamma(1.5) - math.lgamma(m + 1.0))
            for m in range(wave_count)
        ]
    )
    weight = np.sqrt(np.pi * np.cos(phi) / lat_count)
    diagonal = weight[None, :] * np.exp(lead[:, None] + orders[:, None] * np.log(np.cos(phi))[None, :])
    diagonal = diagonal.reshape(groups, pack * half)
    mu = np.broadcast_to(np.tile(np.sin(phi), pack)[None, :], (groups, pack * half))
    degree = orders[:, None]
    above = degree > orders[None, :]
    gap = np.where(above, degree**2 - orders[None, :] ** 2, 1.0)
    up = np.where(above, np.sqrt(np.maximum(4.0 * degree**2 - 1.0, 0.0) / gap), 0.0)
    lower = degree - 1.0
    down = np.sqrt(np.maximum(lower**2 - orders[None, :] ** 2, 0.0) / np.maximum(4.0 * lower**2 - 1.0, 1.0))

    def packed(a):
        a = a.reshape(wave_count // deep, deep, groups, pack)
        return a.transpose(0, 2, 1, 3).reshape(wave_count // deep * groups, deep * pack)

    return [np.asarray(a, np.float32) for a in (mu, diagonal, packed(up), packed(up * down))]


def place_of_device(index):
    sections = lax.axis_size("tm")
    return {"tm": lax.rem(index, sections), "lev": lax.div(index, sections)}


def own_index():
    return lax.axis_index("lev") * lax.axis_size("tm") + lax.axis_index("tm")


def meet():
    count = lax.axis_size("tm") * lax.axis_size("lev")
    me = own_index()
    barrier = pltpu.get_barrier_semaphore()

    def greet(d, carry):
        pl.semaphore_signal(
            barrier, inc=1, device_id=place_of_device(lax.rem(me + d, count)), device_id_type=pl.DeviceIdType.MESH
        )
        return carry

    lax.fori_loop(1, count, greet, 0)
    pl.semaphore_wait(barrier, count - 1)


def rates_for(tangent_ref, rows, section):
    start = jnp.minimum(section * rows, tangent_ref.shape[0] - rows)
    return tangent_ref.at[pl.ds(pl.multiple_of(start, SUBLANES), rows), :]


def rate_copies(source, tangent_ref, place, sent, landed):
    sections = lax.axis_size("tm")
    copies = []
    for d in range(1, sections):
        peer = lax.rem(jnp.int32(source + d), sections)
        copies.append(
            pltpu.make_async_remote_copy(
                src_ref=rates_for(tangent_ref, place.shape[0], peer),
                dst_ref=place,
                send_sem=sent.at[d],
                recv_sem=landed,
                device_id={"tm": peer},
                device_id_type=pl.DeviceIdType.MESH,
            )
        )
    return copies


def bin_shape(lat_rows, lon_cols):
    tall = math.gcd(lat_rows, 32)
    return tall, (lat_rows // tall) * (lon_cols // LANES)


def sort_message(
    lon_cols, tall, bins, mine, cell_ref, innov_ref, damp_ref, out_ref, lane_from, sub_from, swaps
):
    deep = cell_ref.shape[0]
    levels = innov_ref.shape[0] // deep
    sections = out_ref.shape[0]
    blocks = deep // SUBLANES
    low_bits, mid_bits, top_bits = (n.bit_length() - 1 for n in (blocks, SUBLANES, LANES))
    mid_end = low_bits + mid_bits
    all_bits = mid_end + top_bits
    lane = lax.broadcasted_iota(jnp.int32, (SUBLANES, LANES), 1)
    sub = lax.broadcasted_iota(jnp.int32, (SUBLANES, LANES), 0)
    span = tall * LANES
    wide = lon_cols // LANES

    def key_of(cells):
        rows = cells // lon_cols
        cols = cells - rows * lon_cols
        tile = (rows // tall) * wide + cols // LANES
        return tile * span + (rows % tall) * LANES + cols % LANES

    keys = [key_of(cell_ref[v * SUBLANES : (v + 1) * SUBLANES, :]) for v in range(blocks)]

    def falling(stage):
        if stage >= all_bits:
            return None
        if stage >= mid_end:
            return (lane >> (stage - mid_end)) & 1
        return (sub >> (stage - low_bits)) & 1

    plan = []

    def across(values, bits, position, axis, stage, first, last):
        down = falling(stage)
        values = [value * (1 << bits) + position for value in values]
        for bit in range(first, last - 1, -1):
            reach = 1 << bit
            index = position ^ reach
            upper = (position >> bit) & 1
            keep = (upper if down is None else upper ^ down) == 0
            moved = []
            for value in values:
                other = jnp.take_along_axis(value, index, axis=axis, mode="promise_in_bounds")
                moved.append(jnp.where(keep, jnp.minimum(value, other), jnp.maximum(value, other)))
            values = moved
        return [value >> bits for value in values], [value & ((1 << bits) - 1) for value in values]

    for stage in range(1, all_bits + 1):
        if stage > mid_end:
            keys, source = across(keys, top_bits, lane, 1, stage, stage - 1 - mid_end, 0)
            slot = sum(1 for kind, _ in plan if kind == "lane")
            for v in range(blocks):
                lane_from[slot, v] = source[v]
            plan.append(("lane", slot))
        if stage > low_bits:
            keys, source = across(keys, mid_bits, sub, 0, stage, min(stage, mid_end) - 1 - low_bits, 0)
            slot = sum(1 for kind, _ in plan if kind == "sub")
            for v in range(blocks):
                sub_from[slot, v] = source[v]
            plan.append(("sub", slot))
        for bit in range(min(stage, low_bits) - 1, -1, -1):
            down = None if stage < low_bits else falling(stage)
            slot = sum(1 for kind, _ in plan if kind == "swap")
            pair = 0
            for v in range(blocks):
                if v >> bit & 1:
                    continue
                first, second = keys[v], keys[v | 1 << bit]
                if stage < low_bits:
                    swap = first < second if v >> stage & 1 else first > second
                elif down is None:
                    swap = first > second
                else:
                    swap = jnp.where(down == 0, first - second, second - first) > 0
                swaps[slot, pair] = jnp.where(swap, 1, 0)
                keys[v], keys[v | 1 << bit] = jnp.where(swap, second, first), jnp.where(swap, first, second)
                pair += 1
            plan.append(("swap", (slot, bit)))

    for s in range(sections):
        out_ref[s, mine * deep : (mine + 1) * deep, :] = jnp.concatenate([key.astype(F32) for key in keys], 0).T

    edges = jnp.zeros((1, LANES), F32)
    for b in range(1, bins + 1):
        below = sum(jnp.where(key < b * span, 1.0, 0.0) for key in keys)
        below = jnp.sum(jnp.sum(below, 0, keepdims=True), 1, keepdims=True)
        edges = jnp.where(lane[:1] == b, below, edges)
    extra = mine * damp_ref.shape[1] // LANES
    first = lax.axis_index("lev") * levels
    base = (mine + 1) * deep
    for s in range(sections):
        place = jnp.minimum(first + s * mine, damp_ref.shape[0] - mine)
        rows = [damp_ref[pl.ds(place + k, 1), :] for k in range(mine)]
        tail = rows + [edges, jnp.zeros((SUBLANES - extra - 1, LANES), F32)]
        out_ref[s, base : base + SUBLANES, :] = jnp.concatenate(tail, 0)
        for k in range(mine):
            if s * mine + k >= levels:
                out_ref[s, k * deep : (k + 1) * deep, :] = jnp.zeros((deep, LANES), F32)

    def move(p, carry):
        values = [innov_ref[pl.ds(v * SUBLANES * levels + p, SUBLANES, stride=levels), :] for v in range(blocks)]
        for kind, slot in plan:
            if kind == "swap":
                slot, bit = slot
                firsts = [v for v in range(blocks) if not v >> bit & 1]
                for pair, v in enumerate(firsts):
                    swap = swaps[slot, pair] != 0
                    first, second = values[v], values[v | 1 << bit]
                    values[v] = jnp.where(swap, second, first)
                    values[v | 1 << bit] = jnp.where(swap, first, second)
            else:
                ref, axis = (lane_from, 1) if kind == "lane" else (sub_from, 0)
                values = [
                    jnp.take_along_axis(value, ref[slot, v], axis=axis, mode="promise_in_bounds")
                    for v, value in enumerate(values)
                ]
        out_ref[p // mine, pl.ds(pl.multiple_of(p % mine * deep, deep), deep), :] = jnp.concatenate(values, 0).T
        return carry

    lax.fori_loop(0, levels, move, 0)


def forcing_fields(mine, extra, tall, message_ref, out_ref, run_ref, edge_ref, edge_sem):
    times = message_ref.shape[0]
    bins = out_ref.shape[1]
    deep = (message_ref.shape[1] - SUBLANES) // (mine + 1)
    chunks = deep // 2
    span = tall * LANES
    load = pltpu.make_async_copy(message_ref.at[:, (mine + 1) * deep + extra, :], edge_ref, edge_sem)
    load.start()
    run_ref[:, 0] = jnp.zeros(run_ref.shape[:1] + run_ref.shape[2:], F32)
    col_ids = lax.broadcasted_iota(jnp.int32, (LANES, 2 * LANES), 0).astype(F32).astype(BF16)
    row_ids = lax.broadcasted_iota(jnp.int32, (tall, 2 * LANES), 0).astype(F32).astype(BF16)
    one, none = jnp.ones((), BF16), jnp.zeros((), BF16)

    def row_of(t, base, c):
        return jnp.concatenate([message_ref[t, pl.ds(base + 2 * c + i, 1), :] for i in range(2)], 1)

    def visit(t, b, c, live):
        key = row_of(t, mine * deep, c).astype(jnp.int32) - jnp.where(live, b, bins + 1) * span
        cols = (key & (LANES - 1)).astype(F32).astype(BF16)
        rows = (key >> 7).astype(F32).astype(BF16)
        spread_cols = jnp.where(col_ids == jnp.broadcast_to(cols, col_ids.shape), one, none)
        hit = row_ids == jnp.broadcast_to(rows, row_ids.shape)
        parts = [halves(row_of(t, k * deep, c)) for k in range(mine)]
        pieces = [jnp.where(hit, jnp.broadcast_to(part[i], row_ids.shape), none) for i in range(2) for part in parts]
        field = dot(jnp.concatenate(pieces, 0), spread_cols, NT)
        return field[: mine * tall] + field[mine * tall :]

    total = chunks + bins - 1
    unroll = 4
    load.wait()

    def walk(s, state):
        fields, nexts = [], []
        for t in range(times):
            b, c, same = state[t]
            for u in range(unroll):
                place = s * unroll + u
                fields.append((t, place, same, visit(t, b, c, place < total)))
                stay = (edge_ref[t, b + 1].astype(jnp.int32) > (c + 1) * 2 * LANES).astype(jnp.int32)
                after = jnp.minimum(b + 1 - stay, bins - 1)
                same = (after == b).astype(F32)
                b, c = after, jnp.minimum(c + stay, chunks - 1)
            nexts.append((b, c, same))
        for t, place, same, field in fields:
            run_ref[t, place + 1] = run_ref[t, place] * same + field
        return tuple(nexts)

    start = jnp.int32(0)
    steps = -(-total // unroll)
    lax.fori_loop(0, steps, walk, tuple((start, start, jnp.float32(0)) for _ in range(times)))

    def place_bin(b, carry):
        for t in range(times):
            end = edge_ref[t, b + 1].astype(jnp.int32)
            last = b + jnp.maximum((end + 2 * LANES - 1) // (2 * LANES) - 1, 0)
            last = jnp.where(b == bins - 1, steps * unroll - 1, last)
            last = jnp.minimum(jnp.maximum(last, 0), steps * unroll - 1)
            out_ref[t, b] = run_ref[t, last + 1]
        return carry

    lax.fori_loop(0, bins, place_bin, 0)


def lanes_at(value, index):
    return jnp.take_along_axis(value, jnp.broadcast_to(index, value.shape), axis=1, mode="promise_in_bounds")


def legendre_tables(between, half, mu_ref, diag_ref, up_ref, both_ref, high, low, left, right):
    groups, width = mu_ref.shape
    waves = high.shape[1]
    pack = width // half
    deep = LANES // pack
    lane = lax.broadcasted_iota(jnp.int32, (1, LANES), 1)
    sub = lax.broadcasted_iota(jnp.int32, (groups, width), 0)
    orders = sub * pack + lax.broadcasted_iota(jnp.int32, (groups, width), 1) // half

    def advance(n, state):
        one, two = state
        place = pl.ds(pl.multiple_of(n // deep * groups, groups), groups)
        base = (n % deep) * pack

        def spread_out(ref):
            value = ref[place, :]
            return jnp.concatenate([lanes_at(value, base + lane // half + i * (LANES // half)) for i in range(width // LANES)], 1)

        recurred = spread_out(up_ref) * (mu_ref[...] * one) - spread_out(both_ref) * two
        value = jnp.where(orders == n, diag_ref[...], recurred)
        row = (n % 2) * (waves // 2) + n // 2
        left[pl.ds(row, groups, stride=waves), :] = value[:, :LANES]
        right[pl.ds(row, groups, stride=waves), :] = value[:, LANES:]
        return value, one

    zero = 0.0 * mu_ref[...]
    state = lax.fori_loop(0, SUBLANES, advance, (zero, zero), unroll=8)
    between()
    lax.fori_loop(SUBLANES, waves, advance, state, unroll=8)

    def split(g, carry):
        for i, ref in enumerate((left, right)):
            upper, lower = halves(ref[pl.ds(pl.multiple_of(g * waves, waves), waves), :])
            high[g, :, i * LANES : (i + 1) * LANES] = upper
            low[g, :, i * LANES : (i + 1) * LANES] = lower
        return carry

    lax.fori_loop(0, groups, split, 0, unroll=4)


def whole_kernel(
    lon_cols, tall, bins, mine, half,
    cell_ref, innov_ref, damp_ref, mu_ref, diag_ref, up_ref, both_ref, spread_ref, fhigh_ref, flow_ref, tangent_hbm,
    arrived_ref,
    message, received, lane_from, sub_from, swaps, left, right, run_ref, edge_ref,
    field_ref, tail_ref, high, low, tangent_ref, even, odd, packed, total, adjoint, order, outgoing,
    edge_sem, rate_sent, rate_landed, sent, landed, own_sem, spread_sent, spread_landed,
):
    sections = message.shape[0]
    me = lax.axis_index("tm")
    extra = mine * damp_ref.shape[1] // LANES
    deep = cell_ref.shape[0]
    rows = tangent_ref.shape[1]
    own_rates = rates_for(tangent_hbm, rows, me)

    @pl.when(me > 0)
    def _():
        pltpu.make_async_copy(own_rates, tangent_ref.at[me], rate_landed.at[me]).start()

    meet()
    traffic = {
        t: rate_copies(t, tangent_hbm, tangent_ref.at[t], rate_sent, rate_landed.at[t]) for t in range(1, sections)
    }

    def depart(t):
        @pl.when(me == t)
        def _():
            for copy in traffic[t]:
                copy.start()

    depart(sections - 1)
    sort_message(lon_cols, tall, bins, mine, cell_ref, innov_ref, damp_ref, message, lane_from, sub_from, swaps)
    copies = []
    for d in range(1, sections):
        peer = lax.rem(me + d, sections)
        copies.append(
            pltpu.make_async_remote_copy(
                src_ref=message.at[peer],
                dst_ref=received.at[me],
                send_sem=sent.at[d],
                recv_sem=landed.at[d],
                device_id={"tm": peer},
                device_id_type=pl.DeviceIdType.MESH,
            )
        )
    keep = pltpu.make_async_copy(message.at[me], received.at[me], own_sem)

    def between():
        for copy in copies:
            copy.start()
        keep.start()
        for t in range(1, sections - 1):
            depart(t)

    legendre_tables(between, half, mu_ref, diag_ref, up_ref, both_ref, high, low, left, right)
    keep.wait()
    for copy in copies:
        copy.wait()
    base = (mine + 1) * deep
    for t in range(sections):
        tail_ref[t] = received[t, base : base + SUBLANES, :]
    forcing_fields(mine, extra, tall, received, field_ref, run_ref, edge_ref, edge_sem)

    def rates_at(t):
        pltpu.make_async_copy(own_rates, tangent_ref.at[t], rate_landed.at[t]).wait()
        return tangent_ref[t]

    sweep_steps(
        rates_at, field_ref, tail_ref, high, low, spread_ref, fhigh_ref, flow_ref,
        outgoing, even, odd, packed, total, adjoint, order,
    )
    for t, leaving in traffic.items():

        @pl.when(me == t)
        def _():
            for copy in leaving:
                copy.wait_send()

    deal_blocks(outgoing, arrived_ref, spread_sent, spread_landed, own_sem)


def adjoint_totals(cells, innov, damp, spread, tangent, sections, blocks, mine, lat_rows, lon_cols):
    deep = cells.shape[0]
    waves = damp.shape[1]
    columns = deep // SUBLANES
    low_bits, mid_bits, top_bits = (n.bit_length() - 1 for n in (columns, SUBLANES, LANES))
    all_bits = low_bits + mid_bits + top_bits
    tall, bins = bin_shape(lat_rows, lon_cols)
    swap_count = sum(min(stage, low_bits) for stage in range(1, all_bits + 1))
    mu, diagonal, up, both = legendre_coefficients(lat_rows, waves)
    groups, width = mu.shape
    fourier = fourier_rows(lon_cols, waves)
    fhigh = fourier.astype(jnp.bfloat16)
    flow = (fourier - fhigh.astype(np.float32)).astype(jnp.bfloat16)
    message = (sections, (mine + 1) * deep + SUBLANES, LANES)
    places = -(-(deep // 2 + bins - 1) // 4) * 4 + 1
    rows = mine * lat_rows
    group = 4 * mine
    deal = 2 * waves * (waves // sections) // LANES // blocks
    count = blocks * sections
    vmem, anywhere = pl.BlockSpec(memory_space=pltpu.VMEM), pl.BlockSpec(memory_space=pl.ANY)
    return pl.pallas_call(
        functools.partial(whole_kernel, lon_cols, tall, bins, mine, lat_rows // 2),
        in_specs=[vmem] * 10 + [anywhere],
        out_specs=vmem,
        out_shape=jax.ShapeDtypeStruct((count, mine * deal, LANES), F32),
        scratch_shapes=[
            pltpu.VMEM(message, F32),
            pltpu.VMEM(message, F32),
            pltpu.VMEM((top_bits, columns, SUBLANES, LANES), jnp.int32),
            pltpu.VMEM((top_bits + mid_bits, columns, SUBLANES, LANES), jnp.int32),
            pltpu.VMEM((swap_count, max(1, columns // 2), SUBLANES, LANES), jnp.int32),
            pltpu.VMEM((waves * groups, LANES), F32),
            pltpu.VMEM((waves * groups, LANES), F32),
            pltpu.VMEM((sections, places, mine * tall, LANES), F32),
            pltpu.SMEM((sections, LANES), F32),
            pltpu.VMEM((sections, bins, mine * tall, LANES), F32),
            pltpu.VMEM((sections, SUBLANES, LANES), F32),
            pltpu.VMEM((groups, waves, width), BF16),
            pltpu.VMEM((groups, waves, width), BF16),
            pltpu.VMEM((sections, rows, lon_cols), F32),
            pltpu.VMEM((waves * group, LANES), F32),
            pltpu.VMEM((waves * group, LANES), F32),
            pltpu.VMEM((waves * group, LANES), F32),
            pltpu.VMEM((waves * group, LANES), F32),
            pltpu.VMEM((rows, lon_cols), F32),
            pltpu.VMEM((2 * waves, LANES), F32),
            pltpu.VMEM((count, mine * deal, LANES), F32),
            pltpu.SemaphoreType.DMA,
            pltpu.SemaphoreType.DMA((sections,)),
            pltpu.SemaphoreType.DMA((sections,)),
            pltpu.SemaphoreType.DMA((sections,)),
            pltpu.SemaphoreType.DMA((sections,)),
            pltpu.SemaphoreType.DMA,
            pltpu.SemaphoreType.DMA((count,)),
            pltpu.SemaphoreType.DMA((count,)),
        ],
        compiler_params=pltpu.CompilerParams(
            collective_id=0, has_side_effects=True, vmem_limit_bytes=VMEM_BYTES
        ),
        cost_estimate=pl.CostEstimate(flops=2**34, bytes_accessed=2**24, transcendentals=0),
    )(cells, innov, damp, mu, diagonal, up, both, spread, fhigh, flow, tangent)


def deal_blocks(total_ref, out_ref, sent, landed, own_sem):
    count = total_ref.shape[0]
    me = own_index()
    keep = pltpu.make_async_copy(total_ref.at[me], out_ref.at[me], own_sem)

    def copy_to(d):
        peer = lax.rem(me + d, count)
        return pltpu.make_async_remote_copy(
            src_ref=total_ref.at[peer],
            dst_ref=out_ref.at[me],
            send_sem=sent.at[d],
            recv_sem=landed.at[d],
            device_id=place_of_device(peer),
            device_id_type=pl.DeviceIdType.MESH,
        )

    def send(d, carry):
        copy_to(d).start()
        return carry

    def finish(d, carry):
        copy_to(d).wait()
        return carry

    lax.fori_loop(1, count, send, 0)
    keep.start()
    keep.wait()
    lax.fori_loop(1, count, finish, 0)


def sweep_steps(
    rates_at, field_ref, tail_ref, high, low, spread_ref, fhigh_ref, flow_ref,
    out_ref, even, odd, packed, total, adjoint, order,
):
    times = field_ref.shape[0]
    rows, lon_cols = adjoint.shape
    sections = lax.axis_size("tm")
    bins = field_ref.shape[1]
    groups, waves, width = high.shape
    lat_rows = width * groups * 2 // waves
    half = lat_rows // 2
    pack = width // half
    deep = LANES // pack
    levels = rows // lat_rows
    tall = field_ref.shape[2] // levels
    across = lon_cols // LANES
    group = 4 * levels
    mid = group // 2

    lane = lax.broadcasted_iota(jnp.int32, (1, LANES), 1)
    in_first = lane < half
    fold = lane % half
    in_high = lax.broadcasted_iota(jnp.int32, (group, LANES), 0) < mid
    n_even = lax.broadcasted_iota(jnp.int32, (group, LANES), 1) < waves // 2
    lat_south = lax.broadcasted_iota(jnp.int32, (group, LANES), 1) < half
    adjoint[...] = jnp.zeros_like(adjoint)
    total[...] = jnp.zeros_like(total)
    own_half = (lax.broadcasted_iota(jnp.int32, (waves, LANES), 1) // half) == (
        lax.broadcasted_iota(jnp.int32, (waves, LANES), 0) % (LANES // half)
    )

    def damp_of(t):
        index = 2 * (lane % (waves // 2)) + lane // (waves // 2)
        row = lax.broadcasted_iota(jnp.int32, (group, LANES), 0) % mid // 2
        value = jnp.zeros((group, LANES), F32)
        for k in range(levels):
            value = jnp.where(row == k, jnp.broadcast_to(tail_ref[t, k : k + 1, :], value.shape), value)
        return lanes_at(value, index)

    def analyse(t):
        field = [
            jnp.concatenate([field_ref[t, h + i, k * tall : (k + 1) * tall, :] for i in range(across)], 1)
            for k in range(levels)
            for h in range(0, bins, across)
        ]
        forced = adjoint[...] + jnp.concatenate(field, 0)
        adjoint[...] = forced
        upper, lower = halves(forced)
        coeffs = dot(fhigh_ref[...], upper, NT) + dot(flow_ref[...], upper, NT) + dot(fhigh_ref[...], lower, NT)
        for k in range(levels):
            for p in range(2):
                part = coeffs[p * waves : (p + 1) * waves, k * lat_rows : (k + 1) * lat_rows]
                south = lanes_at(part, fold)
                north = lanes_at(part, lat_rows - 1 - fold)
                for value, ref in ((south + north, even), (south - north, odd)):
                    value = jnp.where(own_half, value, 0.0)
                    rounded = value.astype(BF16).astype(F32)
                    ref[pl.ds(2 * k + p, waves, stride=group), :] = rounded
                    ref[pl.ds(mid + 2 * k + p, waves, stride=group), :] = value - rounded

    def pair_sum(value):
        return value + pltpu.roll(value, mid, 0)

    blank = jnp.zeros((group, LANES), F32)
    per_tile = LANES // half

    def place_of(g, i):
        return pl.ds(pl.multiple_of((g * pack + i) * group, group), group)

    def spectral_of(g):
        lefts = []
        for i in range(pack):
            for ref in (even, odd):
                value = ref[place_of(g, i), :]
                tiles = [value if i // per_tile == c else blank for c in range(width // LANES)]
                lefts.append(jnp.concatenate(tiles, 1))
        lefts = jnp.concatenate(lefts, 0).astype(BF16)
        product = dot(lefts, high[g], NT) + dot(lefts, low[g], NT)
        values = []
        for i in range(pack):
            same = product[2 * i * group : (2 * i + 1) * group]
            other = product[(2 * i + 1) * group : (2 * i + 2) * group]
            value = pair_sum(jnp.where(n_even, same, other) if i % 2 == 0 else jnp.where(n_even, other, same))
            total[place_of(g, i), :] += value
            values.append(value)
        return values

    def synthesise(g, values, damp):
        lefts = []
        for i, value in enumerate(values):
            filtered = value * damp
            rounded = filtered.astype(BF16).astype(F32)
            parts = jnp.where(in_high, rounded, filtered - rounded)
            first, second = jnp.where(n_even, parts, 0.0), jnp.where(n_even, 0.0, parts)
            lefts += [first, second] if i % 2 == 0 else [second, first]
        lefts = jnp.concatenate(lefts, 0).astype(BF16)
        product = dot(lefts, high[g], NN) + dot(lefts, low[g], NN)
        for i in range(pack):
            tile = slice(i // per_tile * LANES, (i // per_tile + 1) * LANES)
            same = product[2 * i * group : (2 * i + 1) * group, tile]
            other = product[(2 * i + 1) * group : (2 * i + 2) * group, tile]
            index = (i % per_tile) * half + jnp.where(in_first, lane, lat_rows - 1 - lane)
            same, other = lanes_at(same, index), lanes_at(other, index)
            packed[place_of(g, i), :] = pair_sum(jnp.where(lat_south, same + other, same - other))

    def step(s, carry):
        t = times - 1 - s
        analyse(t)
        damp = damp_of(t)

        def wave(g, inner):
            for i, value in enumerate(spectral_of(g)):
                packed[place_of(g, i), :] = value
            return inner

        def back(g, inner):
            synthesise(g, [packed[place_of(g, i), :] for i in range(pack)], damp)
            return inner

        lax.fori_loop(0, groups, wave, 0, unroll=32)
        lax.fori_loop(0, groups, back, 0, unroll=32)
        synth = jnp.concatenate(
            [
                jnp.concatenate([packed[pl.ds(2 * k + p, waves, stride=group), :] for p in range(2)], 0).T
                for k in range(levels)
            ],
            0,
        )
        upper, lower = halves(synth)
        gridded = dot(upper, fhigh_ref[...], NN) + dot(lower, fhigh_ref[...], NN) + dot(upper, flow_ref[...], NN)
        adjoint[...] = rates_at(t) * adjoint[...] + gridded
        return carry

    lax.fori_loop(0, times - 1, step, 0)
    analyse(0)

    def last(g, inner):
        spectral_of(g)
        return inner

    lax.fori_loop(0, groups, last, 0, unroll=32)

    block_n = waves // sections
    side = LANES // block_n
    deal = 2 * waves // side
    natural = (lane % 2) * (waves // 2) + lane // 2
    lev_dev = spread_ref.shape[0] // lax.axis_size("lev")
    first = lax.axis_index("lev") * lev_dev + lax.axis_index("tm") * levels
    first = jnp.minimum(first, spread_ref.shape[0] - levels)
    for k in range(levels):
        for p in range(2):
            value = total[pl.ds(2 * k + p, waves, stride=group), :]
            order[pl.ds(p, waves, stride=2), :] = lanes_at(value, natural) * spread_ref[pl.ds(first + k, 1), :]
        blocks = [order[pl.ds(q, deal, stride=side), :] for q in range(side)]
        for s in range(sections):
            value = blocks[0] if s == 0 else pltpu.roll(blocks[0], (-s * block_n) % LANES, 1)
            for q in range(1, side):
                moved = blocks[q] if q == s else pltpu.roll(blocks[q], ((q - s) * block_n) % LANES, 1)
                value = jnp.where(lane // block_n == q, moved, value)
            rows = deal * sections // out_ref.shape[0]
            for b in range(out_ref.shape[0] // sections):
                out_ref[b * sections + s, k * rows : (k + 1) * rows, :] = value[b * rows : (b + 1) * rows]


def shards(obs_cell, innovation, tangent, damping, spread, vertical):
    sections = lax.axis_size("tm")
    groups = lax.axis_size("lev")
    lev_dev, lat_rows, lon_cols = tangent.shape[1:]
    levels, waves = damping.shape[1:]
    mine = -(-lev_dev // sections)
    mine += mine % 2
    padded = mine * sections

    deep = obs_cell.shape[1] // LANES
    rates = tangent.reshape(lev_dev * lat_rows, lon_cols)
    innov = innovation.reshape(lev_dev, deep, LANES).transpose(1, 0, 2).reshape(deep * lev_dev, LANES)
    total = adjoint_totals(
        obs_cell.reshape(deep, LANES), innov, damping[0], spread, rates, sections, groups, mine, lat_rows, lon_cols
    )

    block_m = waves // groups
    block_n = waves // sections
    deal = total.shape[1] // mine
    arrived = total.reshape(groups, padded, deal * LANES)[:, :lev_dev].reshape(levels, deal * LANES)
    result = jnp.einsum("kx,kj->xj", arrived, vertical, precision=PRECISE)
    return result.reshape(block_m, 2, block_n, levels).transpose(3, 0, 1, 2)


def solution(mesh):
    placed = (
        P("tm", None),
        P("tm", "lev", None),
        P("tm", "lev", None, None),
        P("tm", None, None),
        P(),
        P(),
    )
    return jax.shard_map(
        shards, mesh=mesh, in_specs=placed, out_specs=P(None, "lev", None, "tm"), check_vma=False
    )
```

```python
import functools
import math

import jax
import jax.numpy as jnp
import numpy as np
from jax import lax
from jax.experimental import pallas as pl
from jax.experimental.pallas import tpu as pltpu
from jax.sharding import PartitionSpec as P

PRECISE = lax.Precision.HIGHEST
BF16 = jnp.bfloat16
F32 = jnp.float32
NT = (((1,), (1,)), ((), ()))
NN = (((1,), (0,)), ((), ()))
VMEM_BYTES = 67043328
LANES = 128
SUBLANES = 8


def dot(left, right, dims):
    return lax.dot_general(left, right, dims, preferred_element_type=F32)


def halves(value):
    high = value.astype(BF16)
    return high, (value - high.astype(F32)).astype(BF16)


def fourier_rows(lon_count, wave_count):
    index = np.arange(wave_count)[:, None] * np.arange(lon_count)[None, :] % lon_count
    angles = 2.0 * np.pi * index / lon_count
    return (np.concatenate([np.cos(angles), np.sin(angles)], 0) * np.sqrt(2.0 / lon_count)).astype(np.float32)


def legendre_coefficients(lat_count, wave_count):
    half = lat_count // 2
    pack = 2 * LANES // half
    groups = wave_count // pack
    deep = LANES // pack
    phi = (np.arange(half) + 0.5) * np.pi / lat_count - 0.5 * np.pi
    orders = np.arange(wave_count).astype(np.float64)
    lead = np.array(
        [
            -0.5 * math.log(2.0)
            + 0.5 * (math.lgamma(m + 1.5) - math.lgamma(1.5) - math.lgamma(m + 1.0))
            for m in range(wave_count)
        ]
    )
    weight = np.sqrt(np.pi * np.cos(phi) / lat_count)
    diagonal = weight[None, :] * np.exp(lead[:, None] + orders[:, None] * np.log(np.cos(phi))[None, :])
    diagonal = diagonal.reshape(groups, pack * half)
    mu = np.broadcast_to(np.tile(np.sin(phi), pack)[None, :], (groups, pack * half))
    degree = orders[:, None]
    above = degree > orders[None, :]
    gap = np.where(above, degree**2 - orders[None, :] ** 2, 1.0)
    up = np.where(above, np.sqrt(np.maximum(4.0 * degree**2 - 1.0, 0.0) / gap), 0.0)
    lower = degree - 1.0
    down = np.sqrt(np.maximum(lower**2 - orders[None, :] ** 2, 0.0) / np.maximum(4.0 * lower**2 - 1.0, 1.0))

    def packed(a):
        a = a.reshape(wave_count // deep, deep, groups, pack)
        return a.transpose(0, 2, 1, 3).reshape(wave_count // deep * groups, deep * pack)

    return [np.asarray(a, np.float32) for a in (mu, diagonal, packed(up), packed(up * down))]


def place_of_device(index):
    sections = lax.axis_size("tm")
    return {"tm": lax.rem(index, sections), "lev": lax.div(index, sections)}


def own_index():
    return lax.axis_index("lev") * lax.axis_size("tm") + lax.axis_index("tm")


def meet():
    count = lax.axis_size("tm") * lax.axis_size("lev")
    me = own_index()
    barrier = pltpu.get_barrier_semaphore()

    def greet(d, carry):
        pl.semaphore_signal(
            barrier, inc=1, device_id=place_of_device(lax.rem(me + d, count)), device_id_type=pl.DeviceIdType.MESH
        )
        return carry

    lax.fori_loop(1, count, greet, 0)
    pl.semaphore_wait(barrier, count - 1)


def rates_for(tangent_ref, rows, section):
    start = jnp.minimum(section * rows, tangent_ref.shape[0] - rows)
    return tangent_ref.at[pl.ds(pl.multiple_of(start, SUBLANES), rows), :]


def rate_copies(source, tangent_ref, place, sent, landed):
    sections = lax.axis_size("tm")
    copies = []
    for d in range(1, sections):
        peer = lax.rem(jnp.int32(source + d), sections)
        copies.append(
            pltpu.make_async_remote_copy(
                src_ref=rates_for(tangent_ref, place.shape[0], peer),
                dst_ref=place,
                send_sem=sent.at[d],
                recv_sem=landed,
                device_id={"tm": peer},
                device_id_type=pl.DeviceIdType.MESH,
            )
        )
    return copies


def bin_shape(lat_rows, lon_cols):
    tall = math.gcd(lat_rows, 32)
    return tall, (lat_rows // tall) * (lon_cols // LANES)


def sort_message(
    lon_cols, tall, bins, mine, target, ready, cell_ref, innov_ref, damp_ref, out_ref, lane_from, sub_from, swaps
):
    deep = cell_ref.shape[0]
    levels = innov_ref.shape[0] // deep
    sections = out_ref.shape[0]
    blocks = deep // SUBLANES
    low_bits, mid_bits, top_bits = (n.bit_length() - 1 for n in (blocks, SUBLANES, LANES))
    mid_end = low_bits + mid_bits
    all_bits = mid_end + top_bits
    lane = lax.broadcasted_iota(jnp.int32, (SUBLANES, LANES), 1)
    sub = lax.broadcasted_iota(jnp.int32, (SUBLANES, LANES), 0)
    span = tall * LANES
    wide = lon_cols // LANES

    def key_of(cells):
        rows = cells // lon_cols
        cols = cells - rows * lon_cols
        tile = (rows // tall) * wide + cols // LANES
        return tile * span + (rows % tall) * LANES + cols % LANES

    keys = [key_of(cell_ref[v * SUBLANES : (v + 1) * SUBLANES, :]) for v in range(blocks)]

    def falling(stage):
        if stage >= all_bits:
            return None
        if stage >= mid_end:
            return (lane >> (stage - mid_end)) & 1
        return (sub >> (stage - low_bits)) & 1

    plan = []

    def across(values, bits, position, axis, stage, first, last):
        down = falling(stage)
        values = [value * (1 << bits) + position for value in values]
        for bit in range(first, last - 1, -1):
            reach = 1 << bit
            index = position ^ reach
            upper = (position >> bit) & 1
            keep = (upper if down is None else upper ^ down) == 0
            moved = []
            for value in values:
                other = jnp.take_along_axis(value, index, axis=axis, mode="promise_in_bounds")
                moved.append(jnp.where(keep, jnp.minimum(value, other), jnp.maximum(value, other)))
            values = moved
        return [value >> bits for value in values], [value & ((1 << bits) - 1) for value in values]

    for stage in range(1, all_bits + 1):
        if stage > mid_end:
            keys, source = across(keys, top_bits, lane, 1, stage, stage - 1 - mid_end, 0)
            slot = sum(1 for kind, _ in plan if kind == "lane")
            for v in range(blocks):
                lane_from[slot, v] = source[v]
            plan.append(("lane", slot))
        if stage > low_bits:
            keys, source = across(keys, mid_bits, sub, 0, stage, min(stage, mid_end) - 1 - low_bits, 0)
            slot = sum(1 for kind, _ in plan if kind == "sub")
            for v in range(blocks):
                sub_from[slot, v] = source[v]
            plan.append(("sub", slot))
        for bit in range(min(stage, low_bits) - 1, -1, -1):
            down = None if stage < low_bits else falling(stage)
            slot = sum(1 for kind, _ in plan if kind == "swap")
            pair = 0
            for v in range(blocks):
                if v >> bit & 1:
                    continue
                first, second = keys[v], keys[v | 1 << bit]
                if stage < low_bits:
                    swap = first < second if v >> stage & 1 else first > second
                elif down is None:
                    swap = first > second
                else:
                    swap = jnp.where(down == 0, first - second, second - first) > 0
                swaps[slot, pair] = jnp.where(swap, 1, 0)
                keys[v], keys[v | 1 << bit] = jnp.where(swap, second, first), jnp.where(swap, first, second)
                pair += 1
            plan.append(("swap", (slot, bit)))

    for s in range(sections):
        out_ref[s, mine * deep : (mine + 1) * deep, :] = jnp.concatenate([key.astype(F32) for key in keys], 0).T

    edges = jnp.zeros((1, LANES), F32)
    for b in range(1, bins + 1):
        below = sum(jnp.where(key < b * span, 1.0, 0.0) for key in keys)
        below = jnp.sum(jnp.sum(below, 0, keepdims=True), 1, keepdims=True)
        edges = jnp.where(lane[:1] == b, below, edges)
    extra = mine * damp_ref.shape[1] // LANES
    first = lax.axis_index("lev") * levels
    base = (mine + 1) * deep
    for s in range(sections):
        place = jnp.minimum(first + s * mine, damp_ref.shape[0] - mine)
        rows = [damp_ref[pl.ds(place + k, 1), :] for k in range(mine)]
        tail = rows + [edges, jnp.zeros((SUBLANES - extra - 1, LANES), F32)]
        out_ref[s, base : base + SUBLANES, :] = jnp.concatenate(tail, 0)

    def move(i, carry):
        ready(i - 1)
        dest, k = target(i)
        p = jnp.minimum(dest * mine + k, levels - 1)
        values = [innov_ref[pl.ds(v * SUBLANES * levels + p, SUBLANES, stride=levels), :] for v in range(blocks)]
        for kind, slot in plan:
            if kind == "swap":
                slot, bit = slot
                firsts = [v for v in range(blocks) if not v >> bit & 1]
                for pair, v in enumerate(firsts):
                    swap = swaps[slot, pair] != 0
                    first, second = values[v], values[v | 1 << bit]
                    values[v] = jnp.where(swap, second, first)
                    values[v | 1 << bit] = jnp.where(swap, first, second)
            else:
                ref, axis = (lane_from, 1) if kind == "lane" else (sub_from, 0)
                values = [
                    jnp.take_along_axis(value, ref[slot, v], axis=axis, mode="promise_in_bounds")
                    for v, value in enumerate(values)
                ]
        block = jnp.concatenate(values, 0).T
        if levels < sections * mine:
            block = block * (dest * mine + k < levels).astype(F32)
        out_ref[dest, pl.ds(pl.multiple_of(k * deep, deep), deep), :] = block
        return carry

    lax.fori_loop(0, sections * mine, move, 0)


def forcing_fields(mine, extra, tall, message_ref, out_ref, run_ref, edge_ref, edge_sem):
    times = message_ref.shape[0]
    bins = out_ref.shape[1]
    deep = (message_ref.shape[1] - SUBLANES) // (mine + 1)
    chunks = deep // 2
    span = tall * LANES
    load = pltpu.make_async_copy(message_ref.at[:, (mine + 1) * deep + extra, :], edge_ref, edge_sem)
    load.start()
    run_ref[:, 0] = jnp.zeros(run_ref.shape[:1] + run_ref.shape[2:], F32)
    col_ids = lax.broadcasted_iota(jnp.int32, (LANES, 2 * LANES), 0).astype(F32).astype(BF16)
    row_ids = lax.broadcasted_iota(jnp.int32, (tall, 2 * LANES), 0).astype(F32).astype(BF16)
    one, none = jnp.ones((), BF16), jnp.zeros((), BF16)

    def row_of(t, base, c):
        return jnp.concatenate([message_ref[t, pl.ds(base + 2 * c + i, 1), :] for i in range(2)], 1)

    def visit(t, b, c, live):
        key = row_of(t, mine * deep, c).astype(jnp.int32) - jnp.where(live, b, bins + 1) * span
        cols = (key & (LANES - 1)).astype(F32).astype(BF16)
        rows = (key >> 7).astype(F32).astype(BF16)
        spread_cols = jnp.where(col_ids == jnp.broadcast_to(cols, col_ids.shape), one, none)
        hit = row_ids == jnp.broadcast_to(rows, row_ids.shape)
        parts = [halves(row_of(t, k * deep, c)) for k in range(mine)]
        pieces = [jnp.where(hit, jnp.broadcast_to(part[i], row_ids.shape), none) for i in range(2) for part in parts]
        field = dot(jnp.concatenate(pieces, 0), spread_cols, NT)
        return field[: mine * tall] + field[mine * tall :]

    total = chunks + bins - 1
    unroll = 8
    load.wait()

    def walk(s, state):
        fields, nexts = [], []
        for t in range(times):
            b, c, same = state[t]
            for u in range(unroll):
                place = s * unroll + u
                fields.append((t, place, same, visit(t, b, c, place < total)))
                stay = (edge_ref[t, b + 1].astype(jnp.int32) > (c + 1) * 2 * LANES).astype(jnp.int32)
                after = jnp.minimum(b + 1 - stay, bins - 1)
                same = (after == b).astype(F32)
                b, c = after, jnp.minimum(c + stay, chunks - 1)
            nexts.append((b, c, same))
        for t, place, same, field in fields:
            run_ref[t, place + 1] = run_ref[t, place] * same + field
        return tuple(nexts)

    start = jnp.int32(0)
    steps = -(-total // unroll)
    lax.fori_loop(0, steps, walk, tuple((start, start, jnp.float32(0)) for _ in range(times)))

    def place_bin(b, carry):
        for t in range(times):
            end = edge_ref[t, b + 1].astype(jnp.int32)
            last = b + jnp.maximum((end + 2 * LANES - 1) // (2 * LANES) - 1, 0)
            last = jnp.where(b == bins - 1, steps * unroll - 1, last)
            last = jnp.minimum(jnp.maximum(last, 0), steps * unroll - 1)
            out_ref[t, b] = run_ref[t, last + 1]
        return carry

    lax.fori_loop(0, bins, place_bin, 0)


def lanes_at(value, index):
    return jnp.take_along_axis(value, jnp.broadcast_to(index, value.shape), axis=1, mode="promise_in_bounds")


def legendre_tables(between, half, mu_ref, diag_ref, up_ref, both_ref, high, low, left, right):
    groups, width = mu_ref.shape
    waves = high.shape[1]
    pack = width // half
    deep = LANES // pack
    lane = lax.broadcasted_iota(jnp.int32, (1, LANES), 1)
    sub = lax.broadcasted_iota(jnp.int32, (groups, width), 0)
    orders = sub * pack + lax.broadcasted_iota(jnp.int32, (groups, width), 1) // half

    def advance(n, state):
        one, two = state
        place = pl.ds(pl.multiple_of(n // deep * groups, groups), groups)
        base = (n % deep) * pack

        def spread_out(ref):
            value = ref[place, :]
            return jnp.concatenate([lanes_at(value, base + lane // half + i * (LANES // half)) for i in range(width // LANES)], 1)

        recurred = spread_out(up_ref) * (mu_ref[...] * one) - spread_out(both_ref) * two
        value = jnp.where(orders == n, diag_ref[...], recurred)
        row = (n % 2) * (waves // 2) + n // 2
        left[pl.ds(row, groups, stride=waves), :] = value[:, :LANES]
        right[pl.ds(row, groups, stride=waves), :] = value[:, LANES:]
        return value, one

    zero = 0.0 * mu_ref[...]
    state = lax.fori_loop(0, SUBLANES, advance, (zero, zero), unroll=8)
    between()
    lax.fori_loop(SUBLANES, waves, advance, state, unroll=8)

    def split(g, carry):
        for i, ref in enumerate((left, right)):
            upper, lower = halves(ref[pl.ds(pl.multiple_of(g * waves, waves), waves), :])
            high[g, :, i * LANES : (i + 1) * LANES] = upper
            low[g, :, i * LANES : (i + 1) * LANES] = lower
        return carry

    lax.fori_loop(0, groups, split, 0, unroll=4)


def whole_kernel(
    lon_cols, tall, bins, mine, half,
    cell_hbm, innov_hbm, damp_hbm, mu_hbm, diag_hbm, up_hbm, both_hbm, spread_hbm, fhigh_hbm, flow_hbm, tangent_hbm,
    arrived_ref,
    cell_ref, innov_ref, damp_ref, mu_ref, diag_ref, up_ref, both_ref, spread_ref, fhigh_ref, flow_ref,
    message, received, lane_from, sub_from, swaps, left, right, run_ref, edge_ref,
    field_ref, tail_ref, high, low, tangent_ref, even, odd, packed, total, adjoint, order, outgoing,
    load_sem, edge_sem, rate_sent, rate_landed, sent, landed, own_sem, spread_sent, spread_landed,
):
    inputs = [
        (cell_hbm, cell_ref), (innov_hbm, innov_ref), (damp_hbm, damp_ref), (mu_hbm, mu_ref), (diag_hbm, diag_ref),
        (up_hbm, up_ref), (both_hbm, both_ref), (spread_hbm, spread_ref), (fhigh_hbm, fhigh_ref), (flow_hbm, flow_ref),
    ]
    sections = message.shape[0]
    me = lax.axis_index("tm")
    extra = mine * damp_ref.shape[1] // LANES
    deep = cell_ref.shape[0]
    rows = tangent_ref.shape[1]
    own_rates = rates_for(tangent_hbm, rows, me)
    loads = [pltpu.make_async_copy(far, near, load_sem.at[i]) for i, (far, near) in enumerate(inputs)]
    for load in loads:
        load.start()

    @pl.when(me > 0)
    def _():
        pltpu.make_async_copy(own_rates, tangent_ref.at[me], rate_landed.at[me]).start()

    meet()
    traffic = {
        t: rate_copies(t, tangent_hbm, tangent_ref.at[t], rate_sent, rate_landed.at[t]) for t in range(1, sections)
    }
    early = (0, sections - 2)

    def depart(t, which):
        @pl.when(me == t)
        def _():
            for i in which:
                traffic[t][i].start()

    depart(sections - 1, early)
    for load in loads[:3]:
        load.wait()
    half_count = sections // 2

    def target(i):
        j, k = i // mine, i % mine
        late = j // half_count
        side = (1 - me // half_count) * (1 - late) + me // half_count * late
        return side * half_count + (me + late + j % half_count) % half_count, k

    def piece_copy(dest, piece):
        size = deep if isinstance(piece, jax.Array) or piece < mine else deep + SUBLANES
        cut = pl.ds(pl.multiple_of(piece * deep, deep), size)
        offset = lax.rem(dest - me + sections, sections)
        return pltpu.make_async_remote_copy(
            src_ref=message.at[dest, cut, :],
            dst_ref=received.at[me, cut, :],
            send_sem=sent.at[offset, piece],
            recv_sem=landed.at[offset, piece],
            device_id={"tm": dest},
            device_id_type=pl.DeviceIdType.MESH,
        )

    def ready(i):
        @pl.when(i == 0)
        def _():
            for d in range(1, sections):
                piece_copy(lax.rem(me + d, sections), mine).start()

        @pl.when(i >= 0)
        def _():
            dest, k = target(i)

            @pl.when(dest != me)
            def _():
                piece_copy(dest, k).start()

    sort_message(
        lon_cols, tall, bins, mine, target, ready, cell_ref, innov_ref, damp_ref, message, lane_from, sub_from, swaps
    )
    keep = pltpu.make_async_copy(message.at[me], received.at[me], own_sem)
    for load in loads[3:]:
        load.wait()

    def between():
        ready(jnp.int32(sections * mine - 1))
        keep.start()
        depart(sections - 1, [i for i in range(sections - 1) if i not in early])
        for t in range(1, sections - 1):
            depart(t, range(sections - 1))

    legendre_tables(between, half, mu_ref, diag_ref, up_ref, both_ref, high, low, left, right)
    keep.wait()
    for d in range(1, sections):
        for piece in range(mine + 1):
            piece_copy(lax.rem(me + d, sections), piece).wait()
    base = (mine + 1) * deep
    for t in range(sections):
        tail_ref[t] = received[t, base : base + SUBLANES, :]
    forcing_fields(mine, extra, tall, received, field_ref, run_ref, edge_ref, edge_sem)

    def rates_at(t):
        pltpu.make_async_copy(own_rates, tangent_ref.at[t], rate_landed.at[t]).wait()
        return tangent_ref[t]

    sweep_steps(
        rates_at, field_ref, tail_ref, high, low, spread_ref, fhigh_ref, flow_ref,
        outgoing, even, odd, packed, total, adjoint, order,
    )
    for t, leaving in traffic.items():

        @pl.when(me == t)
        def _():
            for copy in leaving:
                copy.wait_send()

    deal_blocks(outgoing, arrived_ref, spread_sent, spread_landed, own_sem)


def adjoint_totals(cells, innov, damp, spread, tangent, sections, blocks, mine, lat_rows, lon_cols):
    deep = cells.shape[0]
    waves = damp.shape[1]
    columns = deep // SUBLANES
    low_bits, mid_bits, top_bits = (n.bit_length() - 1 for n in (columns, SUBLANES, LANES))
    all_bits = low_bits + mid_bits + top_bits
    tall, bins = bin_shape(lat_rows, lon_cols)
    swap_count = sum(min(stage, low_bits) for stage in range(1, all_bits + 1))
    mu, diagonal, up, both = legendre_coefficients(lat_rows, waves)
    groups, width = mu.shape
    fourier = fourier_rows(lon_cols, waves)
    fhigh = fourier.astype(jnp.bfloat16)
    flow = (fourier - fhigh.astype(np.float32)).astype(jnp.bfloat16)
    message = (sections, (mine + 1) * deep + SUBLANES, LANES)
    places = -(-(deep // 2 + bins - 1) // 8) * 8 + 1
    rows = mine * lat_rows
    group = 4 * mine
    deal = 2 * waves * (waves // sections) // LANES // blocks
    count = blocks * sections
    inputs = [cells, innov, damp, mu, diagonal, up, both, spread, fhigh, flow]
    vmem, anywhere = pl.BlockSpec(memory_space=pltpu.VMEM), pl.BlockSpec(memory_space=pl.ANY)
    return pl.pallas_call(
        functools.partial(whole_kernel, lon_cols, tall, bins, mine, lat_rows // 2),
        in_specs=[anywhere] * 11,
        out_specs=vmem,
        out_shape=jax.ShapeDtypeStruct((count, mine * deal, LANES), F32),
        scratch_shapes=[pltpu.VMEM(value.shape, value.dtype) for value in inputs]
        + [
            pltpu.VMEM(message, F32),
            pltpu.VMEM(message, F32),
            pltpu.VMEM((top_bits, columns, SUBLANES, LANES), jnp.int32),
            pltpu.VMEM((top_bits + mid_bits, columns, SUBLANES, LANES), jnp.int32),
            pltpu.VMEM((swap_count, max(1, columns // 2), SUBLANES, LANES), jnp.int32),
            pltpu.VMEM((waves * groups, LANES), F32),
            pltpu.VMEM((waves * groups, LANES), F32),
            pltpu.VMEM((sections, places, mine * tall, LANES), F32),
            pltpu.SMEM((sections, LANES), F32),
            pltpu.VMEM((sections, bins, mine * tall, LANES), F32),
            pltpu.VMEM((sections, SUBLANES, LANES), F32),
            pltpu.VMEM((groups, waves, width), BF16),
            pltpu.VMEM((groups, waves, width), BF16),
            pltpu.VMEM((sections, rows, lon_cols), F32),
            pltpu.VMEM((waves * group, LANES), F32),
            pltpu.VMEM((waves * group, LANES), F32),
            pltpu.VMEM((waves * group, LANES), F32),
            pltpu.VMEM((waves * group, LANES), F32),
            pltpu.VMEM((rows, lon_cols), F32),
            pltpu.VMEM((2 * waves, LANES), F32),
            pltpu.VMEM((count, mine * deal, LANES), F32),
            pltpu.SemaphoreType.DMA((len(inputs),)),
            pltpu.SemaphoreType.DMA,
            pltpu.SemaphoreType.DMA((sections,)),
            pltpu.SemaphoreType.DMA((sections,)),
            pltpu.SemaphoreType.DMA((sections, mine + 1)),
            pltpu.SemaphoreType.DMA((sections, mine + 1)),
            pltpu.SemaphoreType.DMA,
            pltpu.SemaphoreType.DMA((count,)),
            pltpu.SemaphoreType.DMA((count,)),
        ],
        compiler_params=pltpu.CompilerParams(
            collective_id=0, has_side_effects=True, vmem_limit_bytes=VMEM_BYTES
        ),
        cost_estimate=pl.CostEstimate(flops=2**34, bytes_accessed=2**24, transcendentals=0),
    )(*inputs, tangent)


def deal_blocks(total_ref, out_ref, sent, landed, own_sem):
    count = total_ref.shape[0]
    me = own_index()
    keep = pltpu.make_async_copy(total_ref.at[me], out_ref.at[me], own_sem)

    def copy_to(d):
        peer = lax.rem(me + d, count)
        return pltpu.make_async_remote_copy(
            src_ref=total_ref.at[peer],
            dst_ref=out_ref.at[me],
            send_sem=sent.at[d],
            recv_sem=landed.at[d],
            device_id=place_of_device(peer),
            device_id_type=pl.DeviceIdType.MESH,
        )

    def send(d, carry):
        copy_to(d).start()
        return carry

    def finish(d, carry):
        copy_to(d).wait()
        return carry

    lax.fori_loop(1, count, send, 0)
    keep.start()
    keep.wait()
    lax.fori_loop(1, count, finish, 0)


def sweep_steps(
    rates_at, field_ref, tail_ref, high, low, spread_ref, fhigh_ref, flow_ref,
    out_ref, even, odd, packed, total, adjoint, order,
):
    times = field_ref.shape[0]
    rows, lon_cols = adjoint.shape
    sections = lax.axis_size("tm")
    bins = field_ref.shape[1]
    groups, waves, width = high.shape
    lat_rows = width * groups * 2 // waves
    half = lat_rows // 2
    pack = width // half
    deep = LANES // pack
    levels = rows // lat_rows
    tall = field_ref.shape[2] // levels
    across = lon_cols // LANES
    group = 4 * levels
    mid = group // 2

    lane = lax.broadcasted_iota(jnp.int32, (1, LANES), 1)
    in_first = lane < half
    fold = lane % half
    in_high = lax.broadcasted_iota(jnp.int32, (group, LANES), 0) < mid
    n_even = lax.broadcasted_iota(jnp.int32, (group, LANES), 1) < waves // 2
    lat_south = lax.broadcasted_iota(jnp.int32, (group, LANES), 1) < half
    adjoint[...] = jnp.zeros_like(adjoint)
    total[...] = jnp.zeros_like(total)
    own_half = (lax.broadcasted_iota(jnp.int32, (waves, LANES), 1) // half) == (
        lax.broadcasted_iota(jnp.int32, (waves, LANES), 0) % (LANES // half)
    )

    def damp_of(t):
        index = 2 * (lane % (waves // 2)) + lane // (waves // 2)
        row = lax.broadcasted_iota(jnp.int32, (group, LANES), 0) % mid // 2
        value = jnp.zeros((group, LANES), F32)
        for k in range(levels):
            value = jnp.where(row == k, jnp.broadcast_to(tail_ref[t, k : k + 1, :], value.shape), value)
        return lanes_at(value, index)

    def analyse(t):
        field = [
            jnp.concatenate([field_ref[t, h + i, k * tall : (k + 1) * tall, :] for i in range(across)], 1)
            for k in range(levels)
            for h in range(0, bins, across)
        ]
        forced = adjoint[...] + jnp.concatenate(field, 0)
        adjoint[...] = forced
        upper, lower = halves(forced)
        coeffs = dot(fhigh_ref[...], upper, NT) + dot(flow_ref[...], upper, NT) + dot(fhigh_ref[...], lower, NT)
        for k in range(levels):
            for p in range(2):
                part = coeffs[p * waves : (p + 1) * waves, k * lat_rows : (k + 1) * lat_rows]
                south = lanes_at(part, fold)
                north = lanes_at(part, lat_rows - 1 - fold)
                for value, ref in ((south + north, even), (south - north, odd)):
                    value = jnp.where(own_half, value, 0.0)
                    rounded = value.astype(BF16).astype(F32)
                    ref[pl.ds(2 * k + p, waves, stride=group), :] = rounded
                    ref[pl.ds(mid + 2 * k + p, waves, stride=group), :] = value - rounded

    def pair_sum(value):
        return value + pltpu.roll(value, mid, 0)

    blank = jnp.zeros((group, LANES), F32)
    per_tile = LANES // half

    def place_of(g, i):
        return pl.ds(pl.multiple_of((g * pack + i) * group, group), group)

    def spectral_of(g):
        lefts = []
        for i in range(pack):
            for ref in (even, odd):
                value = ref[place_of(g, i), :]
                tiles = [value if i // per_tile == c else blank for c in range(width // LANES)]
                lefts.append(jnp.concatenate(tiles, 1))
        lefts = jnp.concatenate(lefts, 0).astype(BF16)
        product = dot(lefts, high[g], NT) + dot(lefts, low[g], NT)
        values = []
        for i in range(pack):
            same = product[2 * i * group : (2 * i + 1) * group]
            other = product[(2 * i + 1) * group : (2 * i + 2) * group]
            value = pair_sum(jnp.where(n_even, same, other) if i % 2 == 0 else jnp.where(n_even, other, same))
            total[place_of(g, i), :] += value
            values.append(value)
        return values

    def synthesise(g, values, damp):
        lefts = []
        for i, value in enumerate(values):
            filtered = value * damp
            rounded = filtered.astype(BF16).astype(F32)
            parts = jnp.where(in_high, rounded, filtered - rounded)
            first, second = jnp.where(n_even, parts, 0.0), jnp.where(n_even, 0.0, parts)
            lefts += [first, second] if i % 2 == 0 else [second, first]
        lefts = jnp.concatenate(lefts, 0).astype(BF16)
        product = dot(lefts, high[g], NN) + dot(lefts, low[g], NN)
        for i in range(pack):
            tile = slice(i // per_tile * LANES, (i // per_tile + 1) * LANES)
            same = product[2 * i * group : (2 * i + 1) * group, tile]
            other = product[(2 * i + 1) * group : (2 * i + 2) * group, tile]
            index = (i % per_tile) * half + jnp.where(in_first, lane, lat_rows - 1 - lane)
            same, other = lanes_at(same, index), lanes_at(other, index)
            packed[place_of(g, i), :] = pair_sum(jnp.where(lat_south, same + other, same - other))

    def step(s, carry):
        t = times - 1 - s
        analyse(t)
        damp = damp_of(t)

        def wave(g, inner):
            for i, value in enumerate(spectral_of(g)):
                packed[place_of(g, i), :] = value
            return inner

        def back(g, inner):
            synthesise(g, [packed[place_of(g, i), :] for i in range(pack)], damp)
            return inner

        lax.fori_loop(0, groups, wave, 0, unroll=32)
        lax.fori_loop(0, groups, back, 0, unroll=32)
        synth = jnp.concatenate(
            [
                jnp.concatenate([packed[pl.ds(2 * k + p, waves, stride=group), :] for p in range(2)], 0).T
                for k in range(levels)
            ],
            0,
        )
        upper, lower = halves(synth)
        gridded = dot(upper, fhigh_ref[...], NN) + dot(lower, fhigh_ref[...], NN) + dot(upper, flow_ref[...], NN)
        adjoint[...] = rates_at(t) * adjoint[...] + gridded
        return carry

    lax.fori_loop(0, times - 1, step, 0)
    analyse(0)

    def last(g, inner):
        spectral_of(g)
        return inner

    lax.fori_loop(0, groups, last, 0, unroll=32)

    block_n = waves // sections
    side = LANES // block_n
    deal = 2 * waves // side
    natural = (lane % 2) * (waves // 2) + lane // 2
    lev_dev = spread_ref.shape[0] // lax.axis_size("lev")
    first = lax.axis_index("lev") * lev_dev + lax.axis_index("tm") * levels
    first = jnp.minimum(first, spread_ref.shape[0] - levels)
    for k in range(levels):
        for p in range(2):
            value = total[pl.ds(2 * k + p, waves, stride=group), :]
            order[pl.ds(p, waves, stride=2), :] = lanes_at(value, natural) * spread_ref[pl.ds(first + k, 1), :]
        blocks = [order[pl.ds(q, deal, stride=side), :] for q in range(side)]
        for s in range(sections):
            value = blocks[0] if s == 0 else pltpu.roll(blocks[0], (-s * block_n) % LANES, 1)
            for q in range(1, side):
                moved = blocks[q] if q == s else pltpu.roll(blocks[q], ((q - s) * block_n) % LANES, 1)
                value = jnp.where(lane // block_n == q, moved, value)
            rows = deal * sections // out_ref.shape[0]
            for b in range(out_ref.shape[0] // sections):
                out_ref[b * sections + s, k * rows : (k + 1) * rows, :] = value[b * rows : (b + 1) * rows]


def shards(obs_cell, innovation, tangent, damping, spread, vertical):
    sections = lax.axis_size("tm")
    groups = lax.axis_size("lev")
    lev_dev, lat_rows, lon_cols = tangent.shape[1:]
    levels, waves = damping.shape[1:]
    mine = -(-lev_dev // sections)
    mine += mine % 2
    padded = mine * sections

    deep = obs_cell.shape[1] // LANES
    rates = tangent.reshape(lev_dev * lat_rows, lon_cols)
    innov = innovation.reshape(lev_dev, deep, LANES).transpose(1, 0, 2).reshape(deep * lev_dev, LANES)
    total = adjoint_totals(
        obs_cell.reshape(deep, LANES), innov, damping[0], spread, rates, sections, groups, mine, lat_rows, lon_cols
    )

    block_m = waves // groups
    block_n = waves // sections
    deal = total.shape[1] // mine
    arrived = total.reshape(groups, padded, deal * LANES)[:, :lev_dev].reshape(levels, deal * LANES)
    result = jnp.einsum("kx,kj->xj", arrived, vertical, precision=PRECISE)
    return result.reshape(block_m, 2, block_n, levels).transpose(3, 0, 1, 2)


def solution(mesh):
    placed = (
        P("tm", None),
        P("tm", "lev", None),
        P("tm", "lev", None, None),
        P("tm", None, None),
        P(),
        P(),
    )
    return jax.shard_map(
        shards, mesh=mesh, in_specs=placed, out_specs=P(None, "lev", None, "tm"), check_vma=False
    )
```

```python
import functools
import math

import jax
import jax.numpy as jnp
import numpy as np
from jax import lax
from jax.experimental import pallas as pl
from jax.experimental.pallas import tpu as pltpu
from jax.sharding import PartitionSpec as P

PRECISE = lax.Precision.HIGHEST
BF16 = jnp.bfloat16
F32 = jnp.float32
NT = (((1,), (1,)), ((), ()))
NN = (((1,), (0,)), ((), ()))
VMEM_BYTES = 67043328
LANES = 128
SUBLANES = 8


def dot(left, right, dims):
    return lax.dot_general(left, right, dims, preferred_element_type=F32)


def halves(value):
    high = value.astype(BF16)
    return high, (value - high.astype(F32)).astype(BF16)


def fourier_rows(lon_count, wave_count):
    index = np.arange(wave_count)[:, None] * np.arange(lon_count)[None, :] % lon_count
    angles = 2.0 * np.pi * index / lon_count
    return (np.concatenate([np.cos(angles), np.sin(angles)], 0) * np.sqrt(2.0 / lon_count)).astype(np.float32)


def legendre_coefficients(lat_count, wave_count):
    half = lat_count // 2
    pack = 2 * LANES // half
    groups = wave_count // pack
    deep = LANES // pack
    phi = (np.arange(half) + 0.5) * np.pi / lat_count - 0.5 * np.pi
    orders = np.arange(wave_count).astype(np.float64)
    lead = np.array(
        [
            -0.5 * math.log(2.0)
            + 0.5 * (math.lgamma(m + 1.5) - math.lgamma(1.5) - math.lgamma(m + 1.0))
            for m in range(wave_count)
        ]
    )
    weight = np.sqrt(np.pi * np.cos(phi) / lat_count)
    diagonal = weight[None, :] * np.exp(lead[:, None] + orders[:, None] * np.log(np.cos(phi))[None, :])
    diagonal = diagonal.reshape(groups, pack * half)
    mu = np.broadcast_to(np.tile(np.sin(phi), pack)[None, :], (groups, pack * half))
    degree = orders[:, None]
    above = degree > orders[None, :]
    gap = np.where(above, degree**2 - orders[None, :] ** 2, 1.0)
    up = np.where(above, np.sqrt(np.maximum(4.0 * degree**2 - 1.0, 0.0) / gap), 0.0)
    lower = degree - 1.0
    down = np.sqrt(np.maximum(lower**2 - orders[None, :] ** 2, 0.0) / np.maximum(4.0 * lower**2 - 1.0, 1.0))

    def packed(a):
        a = a.reshape(wave_count // deep, deep, groups, pack)
        return a.transpose(0, 2, 1, 3).reshape(wave_count // deep * groups, deep * pack)

    return [np.asarray(a, np.float32) for a in (mu, diagonal, packed(up), packed(up * down))]


def place_of_device(index):
    sections = lax.axis_size("tm")
    return {"tm": lax.rem(index, sections), "lev": lax.div(index, sections)}


def own_index():
    return lax.axis_index("lev") * lax.axis_size("tm") + lax.axis_index("tm")


def meet():
    count = lax.axis_size("tm") * lax.axis_size("lev")
    me = own_index()
    barrier = pltpu.get_barrier_semaphore()

    def greet(d, carry):
        pl.semaphore_signal(
            barrier, inc=1, device_id=place_of_device(lax.rem(me + d, count)), device_id_type=pl.DeviceIdType.MESH
        )
        return carry

    lax.fori_loop(1, count, greet, 0)
    pl.semaphore_wait(barrier, count - 1)


def rates_for(tangent_ref, rows, section):
    start = jnp.minimum(section * rows, tangent_ref.shape[0] - rows)
    return tangent_ref.at[pl.ds(pl.multiple_of(start, SUBLANES), rows), :]


def rate_copies(source, tangent_ref, place, sent, landed):
    sections = lax.axis_size("tm")
    copies = []
    for d in range(1, sections):
        peer = lax.rem(jnp.int32(source + d), sections)
        copies.append(
            pltpu.make_async_remote_copy(
                src_ref=rates_for(tangent_ref, place.shape[0], peer),
                dst_ref=place,
                send_sem=sent.at[d],
                recv_sem=landed,
                device_id={"tm": peer},
                device_id_type=pl.DeviceIdType.MESH,
            )
        )
    return copies


def bin_shape(lat_rows, lon_cols):
    tall = math.gcd(lat_rows, 32)
    return tall, (lat_rows // tall) * (lon_cols // LANES)


def sort_message(
    lon_cols, tall, bins, mine, target, ready, cell_ref, innov_ref, damp_ref, out_ref, lane_from, sub_from, swaps
):
    deep = cell_ref.shape[0]
    levels = innov_ref.shape[0] // deep
    sections = out_ref.shape[0]
    blocks = deep // SUBLANES
    low_bits, mid_bits, top_bits = (n.bit_length() - 1 for n in (blocks, SUBLANES, LANES))
    mid_end = low_bits + mid_bits
    all_bits = mid_end + top_bits
    lane = lax.broadcasted_iota(jnp.int32, (SUBLANES, LANES), 1)
    sub = lax.broadcasted_iota(jnp.int32, (SUBLANES, LANES), 0)
    span = tall * LANES
    wide = lon_cols // LANES

    def key_of(cells):
        rows = cells // lon_cols
        cols = cells - rows * lon_cols
        tile = (rows // tall) * wide + cols // LANES
        return tile * span + (rows % tall) * LANES + cols % LANES

    keys = [key_of(cell_ref[v * SUBLANES : (v + 1) * SUBLANES, :]) for v in range(blocks)]

    def falling(stage):
        if stage >= all_bits:
            return None
        if stage >= mid_end:
            return (lane >> (stage - mid_end)) & 1
        return (sub >> (stage - low_bits)) & 1

    plan = []

    def across(values, bits, position, axis, stage, first, last):
        down = falling(stage)
        values = [value * (1 << bits) + position for value in values]
        for bit in range(first, last - 1, -1):
            reach = 1 << bit
            index = position ^ reach
            upper = (position >> bit) & 1
            keep = (upper if down is None else upper ^ down) == 0
            moved = []
            for value in values:
                other = jnp.take_along_axis(value, index, axis=axis, mode="promise_in_bounds")
                moved.append(jnp.where(keep, jnp.minimum(value, other), jnp.maximum(value, other)))
            values = moved
        return [value >> bits for value in values], [value & ((1 << bits) - 1) for value in values]

    for stage in range(1, all_bits + 1):
        if stage > mid_end:
            keys, source = across(keys, top_bits, lane, 1, stage, stage - 1 - mid_end, 0)
            slot = sum(1 for kind, _ in plan if kind == "lane")
            for v in range(blocks):
                lane_from[slot, v] = source[v]
            plan.append(("lane", slot))
        if stage > low_bits:
            keys, source = across(keys, mid_bits, sub, 0, stage, min(stage, mid_end) - 1 - low_bits, 0)
            slot = sum(1 for kind, _ in plan if kind == "sub")
            for v in range(blocks):
                sub_from[slot, v] = source[v]
            plan.append(("sub", slot))
        for bit in range(min(stage, low_bits) - 1, -1, -1):
            down = None if stage < low_bits else falling(stage)
            slot = sum(1 for kind, _ in plan if kind == "swap")
            pair = 0
            for v in range(blocks):
                if v >> bit & 1:
                    continue
                first, second = keys[v], keys[v | 1 << bit]
                if stage < low_bits:
                    swap = first < second if v >> stage & 1 else first > second
                elif down is None:
                    swap = first > second
                else:
                    swap = jnp.where(down == 0, first - second, second - first) > 0
                swaps[slot, pair] = jnp.where(swap, 1, 0)
                keys[v], keys[v | 1 << bit] = jnp.where(swap, second, first), jnp.where(swap, first, second)
                pair += 1
            plan.append(("swap", (slot, bit)))

    for s in range(sections):
        out_ref[s, mine * deep : (mine + 1) * deep, :] = jnp.concatenate([key.astype(F32) for key in keys], 0).T

    edges = jnp.zeros((1, LANES), F32)
    for b in range(1, bins + 1):
        below = sum(jnp.where(key < b * span, 1.0, 0.0) for key in keys)
        below = jnp.sum(jnp.sum(below, 0, keepdims=True), 1, keepdims=True)
        edges = jnp.where(lane[:1] == b, below, edges)
    extra = mine * damp_ref.shape[1] // LANES
    first = lax.axis_index("lev") * levels
    base = (mine + 1) * deep
    for s in range(sections):
        place = jnp.minimum(first + s * mine, damp_ref.shape[0] - mine)
        rows = [damp_ref[pl.ds(place + k, 1), :] for k in range(mine)]
        tail = rows + [edges, jnp.zeros((SUBLANES - extra - 1, LANES), F32)]
        out_ref[s, base : base + SUBLANES, :] = jnp.concatenate(tail, 0)

    def move(j, carry):
        ready(j - 1)
        dest = target(j)
        lists = []
        for k in range(mine):
            p = jnp.minimum(dest * mine + k, levels - 1)
            lists.append(
                [innov_ref[pl.ds(v * SUBLANES * levels + p, SUBLANES, stride=levels), :] for v in range(blocks)]
            )
        for kind, slot in plan:
            if kind == "swap":
                slot, bit = slot
                firsts = [v for v in range(blocks) if not v >> bit & 1]
                for pair, v in enumerate(firsts):
                    swap = swaps[slot, pair] != 0
                    for values in lists:
                        first, second = values[v], values[v | 1 << bit]
                        values[v] = jnp.where(swap, second, first)
                        values[v | 1 << bit] = jnp.where(swap, first, second)
            else:
                ref, axis = (lane_from, 1) if kind == "lane" else (sub_from, 0)
                for v in range(blocks):
                    index = ref[slot, v]
                    for values in lists:
                        values[v] = jnp.take_along_axis(values[v], index, axis=axis, mode="promise_in_bounds")
        for k, values in enumerate(lists):
            block = jnp.concatenate(values, 0).T
            if levels < sections * mine:
                block = block * (dest * mine + k < levels).astype(F32)
            out_ref[dest, k * deep : (k + 1) * deep, :] = block
        return carry

    lax.fori_loop(0, sections, move, 0)


def forcing_fields(mine, extra, tall, message_ref, out_ref, run_ref, edge_ref, edge_sem):
    times = message_ref.shape[0]
    bins = out_ref.shape[1]
    deep = (message_ref.shape[1] - SUBLANES) // (mine + 1)
    chunks = deep // 2
    span = tall * LANES
    load = pltpu.make_async_copy(message_ref.at[:, (mine + 1) * deep + extra, :], edge_ref, edge_sem)
    load.start()
    run_ref[:, 0] = jnp.zeros(run_ref.shape[:1] + run_ref.shape[2:], F32)
    col_ids = lax.broadcasted_iota(jnp.int32, (LANES, 2 * LANES), 0).astype(F32).astype(BF16)
    row_ids = lax.broadcasted_iota(jnp.int32, (tall, 2 * LANES), 0).astype(F32).astype(BF16)
    one, none = jnp.ones((), BF16), jnp.zeros((), BF16)

    def row_of(t, base, c):
        return jnp.concatenate([message_ref[t, pl.ds(base + 2 * c + i, 1), :] for i in range(2)], 1)

    def visit(t, b, c, live):
        key = row_of(t, mine * deep, c).astype(jnp.int32) - jnp.where(live, b, bins + 1) * span
        cols = (key & (LANES - 1)).astype(F32).astype(BF16)
        rows = (key >> 7).astype(F32).astype(BF16)
        spread_cols = jnp.where(col_ids == jnp.broadcast_to(cols, col_ids.shape), one, none)
        hit = row_ids == jnp.broadcast_to(rows, row_ids.shape)
        parts = [halves(row_of(t, k * deep, c)) for k in range(mine)]
        pieces = [jnp.where(hit, jnp.broadcast_to(part[i], row_ids.shape), none) for i in range(2) for part in parts]
        field = dot(jnp.concatenate(pieces, 0), spread_cols, NT)
        return field[: mine * tall] + field[mine * tall :]

    total = chunks + bins - 1
    unroll = 8
    load.wait()

    def walk(s, state):
        fields, nexts = [], []
        for t in range(times):
            b, c, same = state[t]
            for u in range(unroll):
                place = s * unroll + u
                fields.append((t, place, same, visit(t, b, c, place < total)))
                stay = (edge_ref[t, b + 1].astype(jnp.int32) > (c + 1) * 2 * LANES).astype(jnp.int32)
                after = jnp.minimum(b + 1 - stay, bins - 1)
                same = (after == b).astype(F32)
                b, c = after, jnp.minimum(c + stay, chunks - 1)
            nexts.append((b, c, same))
        for t, place, same, field in fields:
            run_ref[t, place + 1] = run_ref[t, place] * same + field
        return tuple(nexts)

    start = jnp.int32(0)
    steps = -(-total // unroll)
    lax.fori_loop(0, steps, walk, tuple((start, start, jnp.float32(0)) for _ in range(times)))

    def place_bin(b, carry):
        for t in range(times):
            end = edge_ref[t, b + 1].astype(jnp.int32)
            last = b + jnp.maximum((end + 2 * LANES - 1) // (2 * LANES) - 1, 0)
            last = jnp.where(b == bins - 1, steps * unroll - 1, last)
            last = jnp.minimum(jnp.maximum(last, 0), steps * unroll - 1)
            out_ref[t, b] = run_ref[t, last + 1]
        return carry

    lax.fori_loop(0, bins, place_bin, 0)


def lanes_at(value, index):
    return jnp.take_along_axis(value, jnp.broadcast_to(index, value.shape), axis=1, mode="promise_in_bounds")


def legendre_tables(between, half, mu_ref, diag_ref, up_ref, both_ref, high, low, left, right):
    groups, width = mu_ref.shape
    waves = high.shape[1]
    pack = width // half
    deep = LANES // pack
    lane = lax.broadcasted_iota(jnp.int32, (1, LANES), 1)
    sub = lax.broadcasted_iota(jnp.int32, (groups, width), 0)
    orders = sub * pack + lax.broadcasted_iota(jnp.int32, (groups, width), 1) // half

    def advance(n, state):
        one, two = state
        place = pl.ds(pl.multiple_of(n // deep * groups, groups), groups)
        base = (n % deep) * pack

        def spread_out(ref):
            value = ref[place, :]
            return jnp.concatenate([lanes_at(value, base + lane // half + i * (LANES // half)) for i in range(width // LANES)], 1)

        recurred = spread_out(up_ref) * (mu_ref[...] * one) - spread_out(both_ref) * two
        value = jnp.where(orders == n, diag_ref[...], recurred)
        row = (n % 2) * (waves // 2) + n // 2
        left[pl.ds(row, groups, stride=waves), :] = value[:, :LANES]
        right[pl.ds(row, groups, stride=waves), :] = value[:, LANES:]
        return value, one

    zero = 0.0 * mu_ref[...]
    state = lax.fori_loop(0, SUBLANES, advance, (zero, zero), unroll=8)
    between()
    lax.fori_loop(SUBLANES, waves, advance, state, unroll=8)

    def split(g, carry):
        for i, ref in enumerate((left, right)):
            upper, lower = halves(ref[pl.ds(pl.multiple_of(g * waves, waves), waves), :])
            high[g, :, i * LANES : (i + 1) * LANES] = upper
            low[g, :, i * LANES : (i + 1) * LANES] = lower
        return carry

    lax.fori_loop(0, groups, split, 0, unroll=4)


def whole_kernel(
    lon_cols, tall, bins, mine, half,
    cell_hbm, innov_hbm, damp_hbm, mu_hbm, diag_hbm, up_hbm, both_hbm, spread_hbm, fhigh_hbm, flow_hbm, vertical_hbm, tangent_hbm,
    result_ref,
    cell_ref, innov_ref, damp_ref, mu_ref, diag_ref, up_ref, both_ref, spread_ref, fhigh_ref, flow_ref, vertical_ref,
    message, received, lane_from, sub_from, swaps, left, right, run_ref, edge_ref,
    field_ref, tail_ref, high, low, tangent_ref, even, odd, packed, total, adjoint, order, outgoing, arrived_ref, flat,
    load_sem, edge_sem, rate_sent, rate_landed, sent, landed, own_sem, spread_sent, spread_landed,
):
    inputs = [
        (cell_hbm, cell_ref), (innov_hbm, innov_ref), (damp_hbm, damp_ref), (mu_hbm, mu_ref), (diag_hbm, diag_ref),
        (up_hbm, up_ref), (both_hbm, both_ref), (spread_hbm, spread_ref), (fhigh_hbm, fhigh_ref), (flow_hbm, flow_ref),
        (vertical_hbm, vertical_ref),
    ]
    sections = message.shape[0]
    me = lax.axis_index("tm")
    extra = mine * damp_ref.shape[1] // LANES
    deep = cell_ref.shape[0]
    rows = tangent_ref.shape[1]
    own_rates = rates_for(tangent_hbm, rows, me)
    loads = [pltpu.make_async_copy(far, near, load_sem.at[i]) for i, (far, near) in enumerate(inputs)]
    for load in loads:
        load.start()

    @pl.when(me > 0)
    def _():
        pltpu.make_async_copy(own_rates, tangent_ref.at[me], rate_landed.at[me]).start()

    meet()
    traffic = {
        t: rate_copies(t, tangent_hbm, tangent_ref.at[t], rate_sent, rate_landed.at[t]) for t in range(1, sections)
    }
    early = (0, sections - 2)

    def depart(t, which):
        @pl.when(me == t)
        def _():
            for i in which:
                traffic[t][i].start()

    depart(sections - 1, early)
    for load in loads[:3]:
        load.wait()
    half_count = sections // 2

    def target(j):
        late = j // half_count
        side = (1 - me // half_count) * (1 - late) + me // half_count * late
        return side * half_count + (me + late + j % half_count) % half_count

    def piece_copy(dest, piece):
        cut = pl.ds(piece * mine * deep, deep + SUBLANES if piece else mine * deep)
        offset = lax.rem(dest - me + sections, sections)
        return pltpu.make_async_remote_copy(
            src_ref=message.at[dest, cut, :],
            dst_ref=received.at[me, cut, :],
            send_sem=sent.at[offset, piece],
            recv_sem=landed.at[offset, piece],
            device_id={"tm": dest},
            device_id_type=pl.DeviceIdType.MESH,
        )

    def ready(j):
        @pl.when(j == 0)
        def _():
            for d in range(1, sections):
                piece_copy(lax.rem(me + d, sections), 1).start()

        @pl.when(j >= 0)
        def _():
            dest = target(j)

            @pl.when(dest != me)
            def _():
                piece_copy(dest, 0).start()

    sort_message(
        lon_cols, tall, bins, mine, target, ready, cell_ref, innov_ref, damp_ref, message, lane_from, sub_from, swaps
    )
    keep = pltpu.make_async_copy(message.at[me], received.at[me], own_sem)
    for load in loads[3:]:
        load.wait()

    def between():
        ready(jnp.int32(sections - 1))
        keep.start()
        depart(sections - 1, [i for i in range(sections - 1) if i not in early])
        for t in range(1, sections - 1):
            depart(t, range(sections - 1))

    legendre_tables(between, half, mu_ref, diag_ref, up_ref, both_ref, high, low, left, right)
    keep.wait()
    for d in range(1, sections):
        for piece in range(2):
            piece_copy(lax.rem(me + d, sections), piece).wait()
    base = (mine + 1) * deep
    for t in range(sections):
        tail_ref[t] = received[t, base : base + SUBLANES, :]
    forcing_fields(mine, extra, tall, received, field_ref, run_ref, edge_ref, edge_sem)

    def rates_at(t):
        pltpu.make_async_copy(own_rates, tangent_ref.at[t], rate_landed.at[t]).wait()
        return tangent_ref[t]

    sweep_steps(
        rates_at, field_ref, tail_ref, high, low, spread_ref, fhigh_ref, flow_ref,
        outgoing, even, odd, packed, total, adjoint, order,
    )
    for t, leaving in traffic.items():

        @pl.when(me == t)
        def _():
            for copy in leaving:
                copy.wait_send()

    deal_blocks(outgoing, arrived_ref, spread_sent, spread_landed, own_sem)
    count, each, _ = arrived_ref.shape
    for i in range(count):
        flat[i * each : (i + 1) * each, :] = arrived_ref[i]
    upper, lower = halves(vertical_ref[...])
    deal = each // mine
    for r in range(deal):
        high_part, low_part = halves(flat[pl.ds(r, count * mine, stride=deal), :].T)
        result_ref[r * LANES : (r + 1) * LANES, :] = (
            dot(high_part, upper, NN) + dot(low_part, upper, NN) + dot(high_part, lower, NN)
        )


def gradient_block(cells, innov, damp, spread, vertical, tangent, sections, blocks, mine, lat_rows, lon_cols):
    deep = cells.shape[0]
    waves = damp.shape[1]
    columns = deep // SUBLANES
    low_bits, mid_bits, top_bits = (n.bit_length() - 1 for n in (columns, SUBLANES, LANES))
    all_bits = low_bits + mid_bits + top_bits
    tall, bins = bin_shape(lat_rows, lon_cols)
    swap_count = sum(min(stage, low_bits) for stage in range(1, all_bits + 1))
    mu, diagonal, up, both = legendre_coefficients(lat_rows, waves)
    groups, width = mu.shape
    fourier = fourier_rows(lon_cols, waves)
    fhigh = fourier.astype(jnp.bfloat16)
    flow = (fourier - fhigh.astype(np.float32)).astype(jnp.bfloat16)
    message = (sections, (mine + 1) * deep + SUBLANES, LANES)
    places = -(-(deep // 2 + bins - 1) // 8) * 8 + 1
    rows = mine * lat_rows
    group = 4 * mine
    deal = 2 * waves * (waves // sections) // LANES // blocks
    count = blocks * sections
    inputs = [cells, innov, damp, mu, diagonal, up, both, spread, fhigh, flow, vertical]
    vmem, anywhere = pl.BlockSpec(memory_space=pltpu.VMEM), pl.BlockSpec(memory_space=pl.ANY)
    return pl.pallas_call(
        functools.partial(whole_kernel, lon_cols, tall, bins, mine, lat_rows // 2),
        in_specs=[anywhere] * (len(inputs) + 1),
        out_specs=vmem,
        out_shape=jax.ShapeDtypeStruct((deal * LANES, vertical.shape[1]), F32),
        scratch_shapes=[pltpu.VMEM(value.shape, value.dtype) for value in inputs]
        + [
            pltpu.VMEM(message, F32),
            pltpu.VMEM(message, F32),
            pltpu.VMEM((top_bits, columns, SUBLANES, LANES), jnp.int32),
            pltpu.VMEM((top_bits + mid_bits, columns, SUBLANES, LANES), jnp.int32),
            pltpu.VMEM((swap_count, max(1, columns // 2), SUBLANES, LANES), jnp.int32),
            pltpu.VMEM((waves * groups, LANES), F32),
            pltpu.VMEM((waves * groups, LANES), F32),
            pltpu.VMEM((sections, places, mine * tall, LANES), F32),
            pltpu.SMEM((sections, LANES), F32),
            pltpu.VMEM((sections, bins, mine * tall, LANES), F32),
            pltpu.VMEM((sections, SUBLANES, LANES), F32),
            pltpu.VMEM((groups, waves, width), BF16),
            pltpu.VMEM((groups, waves, width), BF16),
            pltpu.VMEM((sections, rows, lon_cols), F32),
            pltpu.VMEM((waves * group, LANES), F32),
            pltpu.VMEM((waves * group, LANES), F32),
            pltpu.VMEM((waves * group, LANES), F32),
            pltpu.VMEM((waves * group, LANES), F32),
            pltpu.VMEM((rows, lon_cols), F32),
            pltpu.VMEM((2 * waves, LANES), F32),
            pltpu.VMEM((count, mine * deal, LANES), F32),
            pltpu.VMEM((count, mine * deal, LANES), F32),
            pltpu.VMEM((count * mine * deal, LANES), F32),
            pltpu.SemaphoreType.DMA((len(inputs),)),
            pltpu.SemaphoreType.DMA,
            pltpu.SemaphoreType.DMA((sections,)),
            pltpu.SemaphoreType.DMA((sections,)),
            pltpu.SemaphoreType.DMA((sections, 2)),
            pltpu.SemaphoreType.DMA((sections, 2)),
            pltpu.SemaphoreType.DMA,
            pltpu.SemaphoreType.DMA((count,)),
            pltpu.SemaphoreType.DMA((count,)),
        ],
        compiler_params=pltpu.CompilerParams(
            collective_id=0, has_side_effects=True, vmem_limit_bytes=VMEM_BYTES
        ),
        cost_estimate=pl.CostEstimate(flops=2**34, bytes_accessed=2**24, transcendentals=0),
    )(*inputs, tangent)


def deal_blocks(total_ref, out_ref, sent, landed, own_sem):
    count = total_ref.shape[0]
    me = own_index()
    keep = pltpu.make_async_copy(total_ref.at[me], out_ref.at[me], own_sem)

    def copy_to(d):
        peer = lax.rem(me + d, count)
        return pltpu.make_async_remote_copy(
            src_ref=total_ref.at[peer],
            dst_ref=out_ref.at[me],
            send_sem=sent.at[d],
            recv_sem=landed.at[d],
            device_id=place_of_device(peer),
            device_id_type=pl.DeviceIdType.MESH,
        )

    def send(d, carry):
        copy_to(d).start()
        return carry

    def finish(d, carry):
        copy_to(d).wait()
        return carry

    lax.fori_loop(1, count, send, 0)
    keep.start()
    keep.wait()
    lax.fori_loop(1, count, finish, 0)


def sweep_steps(
    rates_at, field_ref, tail_ref, high, low, spread_ref, fhigh_ref, flow_ref,
    out_ref, even, odd, packed, total, adjoint, order,
):
    times = field_ref.shape[0]
    rows, lon_cols = adjoint.shape
    sections = lax.axis_size("tm")
    bins = field_ref.shape[1]
    groups, waves, width = high.shape
    lat_rows = width * groups * 2 // waves
    half = lat_rows // 2
    pack = width // half
    deep = LANES // pack
    levels = rows // lat_rows
    tall = field_ref.shape[2] // levels
    across = lon_cols // LANES
    group = 4 * levels
    mid = group // 2

    lane = lax.broadcasted_iota(jnp.int32, (1, LANES), 1)
    in_first = lane < half
    fold = lane % half
    in_high = lax.broadcasted_iota(jnp.int32, (group, LANES), 0) < mid
    n_even = lax.broadcasted_iota(jnp.int32, (group, LANES), 1) < waves // 2
    lat_south = lax.broadcasted_iota(jnp.int32, (group, LANES), 1) < half
    adjoint[...] = jnp.zeros_like(adjoint)
    total[...] = jnp.zeros_like(total)
    own_half = (lax.broadcasted_iota(jnp.int32, (waves, LANES), 1) // half) == (
        lax.broadcasted_iota(jnp.int32, (waves, LANES), 0) % (LANES // half)
    )

    def damp_of(t):
        index = 2 * (lane % (waves // 2)) + lane // (waves // 2)
        row = lax.broadcasted_iota(jnp.int32, (group, LANES), 0) % mid // 2
        value = jnp.zeros((group, LANES), F32)
        for k in range(levels):
            value = jnp.where(row == k, jnp.broadcast_to(tail_ref[t, k : k + 1, :], value.shape), value)
        return lanes_at(value, index)

    def analyse(t):
        field = [
            jnp.concatenate([field_ref[t, h + i, k * tall : (k + 1) * tall, :] for i in range(across)], 1)
            for k in range(levels)
            for h in range(0, bins, across)
        ]
        forced = adjoint[...] + jnp.concatenate(field, 0)
        adjoint[...] = forced
        upper, lower = halves(forced)
        coeffs = dot(fhigh_ref[...], upper, NT) + dot(flow_ref[...], upper, NT) + dot(fhigh_ref[...], lower, NT)
        for k in range(levels):
            for p in range(2):
                part = coeffs[p * waves : (p + 1) * waves, k * lat_rows : (k + 1) * lat_rows]
                south = lanes_at(part, fold)
                north = lanes_at(part, lat_rows - 1 - fold)
                for value, ref in ((south + north, even), (south - north, odd)):
                    value = jnp.where(own_half, value, 0.0)
                    rounded = value.astype(BF16).astype(F32)
                    ref[pl.ds(2 * k + p, waves, stride=group), :] = rounded
                    ref[pl.ds(mid + 2 * k + p, waves, stride=group), :] = value - rounded

    def pair_sum(value):
        return value + pltpu.roll(value, mid, 0)

    blank = jnp.zeros((group, LANES), F32)
    per_tile = LANES // half

    def place_of(g, i):
        return pl.ds(pl.multiple_of((g * pack + i) * group, group), group)

    def spectral_of(g):
        lefts = []
        for i in range(pack):
            for ref in (even, odd):
                value = ref[place_of(g, i), :]
                tiles = [value if i // per_tile == c else blank for c in range(width // LANES)]
                lefts.append(jnp.concatenate(tiles, 1))
        lefts = jnp.concatenate(lefts, 0).astype(BF16)
        product = dot(lefts, high[g], NT) + dot(lefts, low[g], NT)
        values = []
        for i in range(pack):
            same = product[2 * i * group : (2 * i + 1) * group]
            other = product[(2 * i + 1) * group : (2 * i + 2) * group]
            value = pair_sum(jnp.where(n_even, same, other) if i % 2 == 0 else jnp.where(n_even, other, same))
            total[place_of(g, i), :] += value
            values.append(value)
        return values

    def synthesise(g, values, damp):
        lefts = []
        for i, value in enumerate(values):
            filtered = value * damp
            rounded = filtered.astype(BF16).astype(F32)
            parts = jnp.where(in_high, rounded, filtered - rounded)
            first, second = jnp.where(n_even, parts, 0.0), jnp.where(n_even, 0.0, parts)
            lefts += [first, second] if i % 2 == 0 else [second, first]
        lefts = jnp.concatenate(lefts, 0).astype(BF16)
        product = dot(lefts, high[g], NN) + dot(lefts, low[g], NN)
        for i in range(pack):
            tile = slice(i // per_tile * LANES, (i // per_tile + 1) * LANES)
            same = product[2 * i * group : (2 * i + 1) * group, tile]
            other = product[(2 * i + 1) * group : (2 * i + 2) * group, tile]
            index = (i % per_tile) * half + jnp.where(in_first, lane, lat_rows - 1 - lane)
            same, other = lanes_at(same, index), lanes_at(other, index)
            packed[place_of(g, i), :] = pair_sum(jnp.where(lat_south, same + other, same - other))

    def step(s, carry):
        t = times - 1 - s
        analyse(t)
        damp = damp_of(t)

        def wave(g, inner):
            for i, value in enumerate(spectral_of(g)):
                packed[place_of(g, i), :] = value
            return inner

        def back(g, inner):
            synthesise(g, [packed[place_of(g, i), :] for i in range(pack)], damp)
            return inner

        lax.fori_loop(0, groups, wave, 0, unroll=32)
        lax.fori_loop(0, groups, back, 0, unroll=32)
        synth = jnp.concatenate(
            [
                jnp.concatenate([packed[pl.ds(2 * k + p, waves, stride=group), :] for p in range(2)], 0).T
                for k in range(levels)
            ],
            0,
        )
        upper, lower = halves(synth)
        gridded = dot(upper, fhigh_ref[...], NN) + dot(lower, fhigh_ref[...], NN) + dot(upper, flow_ref[...], NN)
        adjoint[...] = rates_at(t) * adjoint[...] + gridded
        return carry

    lax.fori_loop(0, times - 1, step, 0)
    analyse(0)

    def last(g, inner):
        spectral_of(g)
        return inner

    lax.fori_loop(0, groups, last, 0, unroll=32)

    block_n = waves // sections
    side = LANES // block_n
    deal = 2 * waves // side
    natural = (lane % 2) * (waves // 2) + lane // 2
    lev_dev = spread_ref.shape[0] // lax.axis_size("lev")
    first = lax.axis_index("lev") * lev_dev + lax.axis_index("tm") * levels
    first = jnp.minimum(first, spread_ref.shape[0] - levels)
    for k in range(levels):
        for p in range(2):
            value = total[pl.ds(2 * k + p, waves, stride=group), :]
            order[pl.ds(p, waves, stride=2), :] = lanes_at(value, natural) * spread_ref[pl.ds(first + k, 1), :]
        blocks = [order[pl.ds(q, deal, stride=side), :] for q in range(side)]
        for s in range(sections):
            value = blocks[0] if s == 0 else pltpu.roll(blocks[0], (-s * block_n) % LANES, 1)
            for q in range(1, side):
                moved = blocks[q] if q == s else pltpu.roll(blocks[q], ((q - s) * block_n) % LANES, 1)
                value = jnp.where(lane // block_n == q, moved, value)
            rows = deal * sections // out_ref.shape[0]
            for b in range(out_ref.shape[0] // sections):
                out_ref[b * sections + s, k * rows : (k + 1) * rows, :] = value[b * rows : (b + 1) * rows]


def shards(obs_cell, innovation, tangent, damping, spread, vertical):
    sections = lax.axis_size("tm")
    groups = lax.axis_size("lev")
    lev_dev, lat_rows, lon_cols = tangent.shape[1:]
    levels, waves = damping.shape[1:]
    mine = -(-lev_dev // sections)
    mine += mine % 2
    padded = mine * sections

    deep = obs_cell.shape[1] // LANES
    rates = tangent.reshape(lev_dev * lat_rows, lon_cols)
    innov = innovation.reshape(lev_dev, deep, LANES).transpose(1, 0, 2).reshape(deep * lev_dev, LANES)
    mixing = vertical
    if padded > lev_dev:
        mixing = vertical.reshape(groups, lev_dev, levels)
        mixing = jnp.pad(mixing, ((0, 0), (0, padded - lev_dev), (0, 0))).reshape(groups * padded, levels)
    result = gradient_block(
        obs_cell.reshape(deep, LANES), innov, damping[0], spread, mixing, rates, sections, groups, mine, lat_rows, lon_cols
    )

    block_m = waves // groups
    block_n = waves // sections
    return result.reshape(block_m, 2, block_n, levels).transpose(3, 0, 1, 2)


def solution(mesh):
    placed = (
        P("tm", None),
        P("tm", "lev", None),
        P("tm", "lev", None, None),
        P("tm", None, None),
        P(),
        P(),
    )
    return jax.shard_map(
        shards, mesh=mesh, in_specs=placed, out_specs=P(None, "lev", None, "tm"), check_vma=False
    )
```
